256 devices in a mesh: gx: 4 (over x), gz: 64 (over z, y, core).
Axes of the slice: x: 4, y: 4, z: 8, core: 2. Of those that a mesh axis runs over, the one named last changes fastest.
Arguments:
- velocity: float32 [3, 64, 256, 512], P(None, 'gz', None, 'gx'), may hold values from -3.5 to 3.5
- earlier_term: bfloat16 [3, 64, 256, 512], P(None, 'gz', None, 'gx'), may hold values from -4 to 4
- face_metric: float32 [2, 64], replicated, may hold values from 0.5 to 2, as said below
Outputs:
- new_velocity: float32 [3, 64, 256, 512], P(None, 'gz', None, 'gx')
- pressure: float32 [64, 256, 512], P('gz', None, 'gx')
The draws below stay inside these ranges and needn't reach their ends.
Inputs may be any that keep to these rules, and one draw needn't show every extreme that they name: face_metric[1, k] equals face_metric[0, k + 1].
All inputs are finite; a program needn't handle non-finite values.
Results may differ from the reference program's by a relative error of at most 0.0012.
Values sent between devices are 32-bit elements; how exact they have to be, the bound alone decides.
A program may use at most 64 MiB of HBM per device.

```python
import math
import jax
import jax.numpy as jnp
from jax import lax

NX = 512
NY = 256
NZ = 64


def draw_velocity(key, part):
    noise_key = jax.random.fold_in(jax.random.fold_in(key, 11), 0)
    grid_shape = (3, NZ, NY, NX)
    values = jnp.clip(jax.random.normal(noise_key, grid_shape, jnp.float32), -3.5, 3.5)
    return values


def draw_face_metric(key, part):
    face_key = jax.random.fold_in(key, 23)
    spread = jax.random.uniform(face_key, (NZ + 1,), jnp.float32)
    face_values = 0.5 * jnp.exp(spread * math.log(4.0))
    return jnp.stack([face_values[:-1], face_values[1:]])


def shard_levels(rng, dims, cuts, smallest, top_value):
    factor_of = 1.0
    for axis_at, parts in cuts:
        steps = jax.random.uniform(jax.random.fold_in(jax.random.fold_in(rng, 6), axis_at), (parts,), jnp.float32, smallest / len(cuts), top_value / len(cuts))
        factor_of = factor_of * jnp.repeat(jnp.exp(steps), dims[axis_at] // parts).reshape((-1,) + (1,) * (len(dims) - 1 - axis_at))
    return factor_of


def gaussian(key, shape, deviation, reach, pieces=(), kind=jnp.bfloat16):
    array = jax.random.normal(key, shape, jnp.float32) * deviation
    if len(pieces) > 0:
        array = shard_levels(key, shape, pieces, -0.22, 0.18) * array
    return jnp.clip(array, min=-reach, max=reach).astype(kind)


def setup_inputs(seed: int = 0) -> dict:
    key_list = jax.random.split(jax.random.key(seed), 4)
    velocity = draw_velocity(jax.random.fold_in(key_list[3], 71), 0)
    earlier_term = gaussian(key_list[1], (3, NZ, NY, NX), 1.0, 4.0, ((1, 64), (3, 4)))
    face_metric = draw_face_metric(jax.random.fold_in(key_list[3], 71), 0)
    return {"velocity": velocity, "earlier_term": earlier_term, "face_metric": face_metric}


TIME_STEP = 0.4
ADVECT_WEIGHT = 5.0 / 12.0
EARLIER_WEIGHT = -17.0 / 60.0
VISCOUS_WEIGHT = 2.0 / 15.0

def cosine_forward(values, axis):
    moved_axis = jnp.moveaxis(values, axis, -1)
    extent = moved_axis.shape[-1]
    mirrored = jnp.concatenate([moved_axis, jnp.flip(moved_axis, -1)], -1)
    spectrum = jnp.fft.fft(mirrored)[..., :extent]
    wave_index = jnp.arange(extent, dtype=jnp.float32)
    twiddle = jnp.exp(-1j * math.pi * wave_index / (2 * extent))
    result = jnp.real(spectrum * twiddle) * (0.5 * math.sqrt(2.0 / extent))
    result = result.at[..., 0].multiply(math.sqrt(0.5))
    return jnp.moveaxis(result.astype(values.dtype), -1, axis)

def cosine_inverse(values, axis):
    moved_axis = jnp.moveaxis(values, axis, -1)
    extent = moved_axis.shape[-1]
    wave_index = jnp.arange(extent, dtype=jnp.float32)
    weights = jnp.ones_like(wave_index).at[0].set(math.sqrt(0.5)) * math.sqrt(2.0 / extent)
    twiddle = jnp.exp(1j * math.pi * wave_index / (2 * extent))
    rotated = moved_axis * weights * twiddle
    padded = jnp.concatenate([rotated, jnp.zeros_like(rotated)], -1)
    result = jnp.real(jnp.fft.ifft(padded))[..., :extent] * (2 * extent)
    return jnp.moveaxis(result.astype(values.dtype), -1, axis)

def wave_squares(extent):
    return (jnp.arange(extent, dtype=jnp.float32) * (math.pi / extent)) ** 2

def along_y(field):
    y_after = jnp.concatenate([field[..., 1:, :], field[..., -1:, :]], -2)
    y_before = jnp.concatenate([field[..., :1, :], field[..., :-1, :]], -2)
    return (y_after, y_before)

def along_z(field):
    z_after = jnp.concatenate([field[..., 1:, :, :], jnp.zeros_like(field[..., :1, :, :])], -3)
    z_before = jnp.concatenate([jnp.zeros_like(field[..., :1, :, :]), field[..., :-1, :, :]], -3)
    return (z_after, z_before)

def reference(velocity, earlier_term, face_metric):
    lower_face = face_metric[0][:, None, None]
    upper_face = face_metric[1][:, None, None]
    metric = 0.5 * (lower_face + upper_face)
    y_squares = wave_squares(NY)
    x_squares = wave_squares(NX)
    x_after = jnp.roll(velocity, -1, -1)
    x_before = jnp.roll(velocity, 1, -1)
    y_after, y_before = along_y(velocity)
    z_after, z_before = along_z(velocity)
    grad_x = 0.5 * (x_after - x_before)
    grad_y = 0.5 * (y_after - y_before)
    grad_z = metric * (0.5 * (z_after - z_before))
    lap_x = x_after + x_before - 2.0 * velocity
    lap_z = metric * (upper_face * (z_after - velocity) - lower_face * (velocity - z_before))

    def plane_diffusion(plane):
        return cosine_inverse(-y_squares[:, None] * cosine_forward(plane, 0), 0)
    lap_y = lax.map(plane_diffusion, velocity.reshape(-1, NY, NX)).reshape(velocity.shape)
    advect = velocity[0:1] * grad_x + velocity[1:2] * grad_y + velocity[2:3] * grad_z
    predicted = velocity + TIME_STEP * (-ADVECT_WEIGHT * advect + EARLIER_WEIGHT * earlier_term.astype(jnp.float32) + VISCOUS_WEIGHT * (lap_x + lap_y + lap_z))
    u_pred = predicted[0]
    v_after, v_before = along_y(predicted[1])
    w_after, w_before = along_z(predicted[2])
    divergence = 0.5 * (jnp.roll(u_pred, -1, -1) - jnp.roll(u_pred, 1, -1)) + 0.5 * (v_after - v_before) + metric * (0.5 * (w_after - w_before))
    source = divergence / TIME_STEP

    def plane_forward(plane):
        return cosine_forward(cosine_forward(plane, 0), 1)
    coeffs = lax.map(plane_forward, source)
    eigen_sum = y_squares[:, None] + x_squares[None, :]
    metric_rows = 0.5 * (face_metric[0] + face_metric[1])

    def forward_step(state_pair, row_data):
        ratio_c, ratio_d = state_pair
        lower_row, upper_row, metric_row, source_row = row_data
        diagonal = -(lower_row + upper_row) - eigen_sum / metric_row
        pivots = diagonal - lower_row * ratio_c
        new_c = upper_row / pivots
        new_d = (source_row / metric_row - lower_row * ratio_d) / pivots
        return ((new_c, new_d), (new_c, new_d))
    empty = jnp.zeros_like(coeffs[0])
    _, (ratios_c, ratios_d) = lax.scan(forward_step, (empty, empty), (face_metric[0], face_metric[1], metric_rows, coeffs))

    def backward_step(following, row_data):
        ratio_c, ratio_d = row_data
        value = ratio_d - ratio_c * following
        return (value, value)
    _, solved = lax.scan(backward_step, empty, (ratios_c, ratios_d), reverse=True)

    def plane_inverse(plane):
        return cosine_inverse(cosine_inverse(plane, 1), 0)
    pressure = lax.map(plane_inverse, solved)
    p_after, p_before = along_y(pressure)
    pz_after, pz_before = along_z(pressure)
    press_x = 0.5 * (jnp.roll(pressure, -1, -1) - jnp.roll(pressure, 1, -1))
    press_y = 0.5 * (p_after - p_before)
    press_z = metric * (0.5 * (pz_after - pz_before))
    new_velocity = predicted - TIME_STEP * jnp.stack([press_x, press_y, press_z])
    return (new_velocity, pressure)
```

```python
import math

import jax
import jax.numpy as jnp
from jax import lax
from jax.experimental import pallas as pl
from jax.experimental.pallas import tpu as pltpu
from jax.sharding import PartitionSpec as P

TIME_STEP = 0.4
ADVECT_WEIGHT = 5.0 / 12.0
EARLIER_WEIGHT = -17.0 / 60.0
VISCOUS_WEIGHT = 2.0 / 15.0


def padded(cells, sides, width, closed):
    for axis, dim in sides:
        count = lax.axis_size(axis)
        ends = count if closed else count - 1
        head = lax.slice_in_dim(cells, 0, width, axis=dim)
        tail = lax.slice_in_dim(cells, cells.shape[dim] - width, cells.shape[dim], axis=dim)
        cells = jnp.concatenate(
            [
                lax.ppermute(tail, axis, [(i, (i + 1) % count) for i in range(ends)]),
                cells,
                lax.ppermute(head, axis, [((i + 1) % count, i) for i in range(ends)]),
            ],
            axis=dim,
        )
    return cells


def cosine_table(extent):
    wavenumber = jnp.arange(extent, dtype=jnp.int32)[:, None]
    points = jnp.arange(extent, dtype=jnp.int32)[None, :]
    residue = wavenumber * (2 * points + 1) % (4 * extent)
    cosines = jnp.cos(residue.astype(jnp.float32) * (math.pi / (2 * extent))) * math.sqrt(
        2.0 / extent
    )
    return cosines.at[0].multiply(math.sqrt(0.5))


def wave_squares(extent):
    return (jnp.arange(extent, dtype=jnp.float32) * (math.pi / extent)) ** 2


def transform_y(cosines, field):
    return jnp.einsum("jy,zyx->zjx", cosines, field, precision=lax.Precision.HIGHEST)


def inverse_y(cosines, field):
    return jnp.einsum("jy,zjx->zyx", cosines, field, precision=lax.Precision.HIGHEST)


def neighbours_y(field):
    y_after = jnp.concatenate([field[..., 1:, :], field[..., -1:, :]], -2)
    y_before = jnp.concatenate([field[..., :1, :], field[..., :-1, :]], -2)
    return (y_after, y_before)


LOGICAL = pl.DeviceIdType.LOGICAL


def relative_devices(group, layer):
    z_parts = [((layer & 56) + (shift << 3)) & 56 for shift in range(8)]
    y_parts = [((layer & 6) + (shift << 1)) & 6 for shift in range(4)]
    core_parts = [layer & 1, (layer & 1) ^ 1]
    x_parts = [(group + shift) & 3 for shift in range(4)]
    order = [
        (i, j, k, m)
        for j in (4, 3, 5, 2, 6, 1, 7, 0)
        for k in (2, 1, 3, 0)
        for i in (2, 1, 3, 0)
        for m in (1, 0)
    ]
    return [
        (x_parts[i], z_parts[j] | y_parts[k] | core_parts[m])
        for i, j, k, m in order
        if (i, j, k, m) != (0, 0, 0, 0)
    ]


def spectral_kernel(
    faces,
    y_rows,
    x_cosines,
    out_rows,
    gathered,
    spread,
    factor_c,
    factor_a,
    factor_b,
    send_a,
    recv_a,
    send_b,
    recv_b,
):
    group = lax.axis_index("gx")
    layer = lax.axis_index("gz")
    me = group * 64 + layer
    others = relative_devices(group, layer)
    barrier = pltpu.get_barrier_semaphore()
    for px, pz in others:
        pl.semaphore_signal(barrier, inc=1, device_id=px * 64 + pz, device_id_type=LOGICAL)
    pl.semaphore_wait(barrier, 255)
    for px, pz in others:
        peer = px * 64 + pz
        pltpu.make_async_remote_copy(
            src_ref=y_rows.at[pl.ds(peer, 1)],
            dst_ref=gathered.at[group, pl.ds(layer, 1)],
            send_sem=send_a,
            recv_sem=recv_a,
            device_id=peer,
            device_id_type=LOGICAL,
        ).start()
    gathered[group, pl.ds(layer, 1)] = y_rows[pl.ds(me, 1)]
    k_y = me.astype(jnp.float32) * (math.pi / 256)
    k_x = lax.broadcasted_iota(jnp.int32, (1, 512), 1).astype(jnp.float32) * (math.pi / 512)
    eigen = k_y * k_y + k_x * k_x
    ratio = jnp.zeros((1, 512), jnp.float32)
    for z in range(64):
        lower = faces[0, z]
        upper = faces[1, z]
        per_metric = 2.0 / jnp.full((1, 512), lower + upper, jnp.float32)
        inverse = 1.0 / (-(lower + upper) - eigen * per_metric - lower * ratio)
        ratio = upper * inverse
        factor_c[pl.ds(z, 1)] = ratio
        factor_a[pl.ds(z, 1)] = lower * inverse
        factor_b[pl.ds(z, 1)] = per_metric * inverse
    rows = y_rows.at[pl.ds(0, 255)]
    pltpu.make_async_copy(rows, rows, recv_a).wait()
    coeffs = jnp.zeros((64, 512), jnp.float32)
    for part in range(4):
        coeffs = coeffs + lax.dot_general(
            gathered[part],
            x_cosines[:, part * 128 : part * 128 + 128],
            (((1,), (1,)), ((), ())),
            precision=lax.Precision.HIGHEST,
            preferred_element_type=jnp.float32,
        )
    factor_b[...] = factor_b[...] * coeffs
    value = jnp.zeros((1, 512), jnp.float32)
    for z in range(64):
        value = factor_b[pl.ds(z, 1)] - factor_a[pl.ds(z, 1)] * value
        factor_b[pl.ds(z, 1)] = value
    value = jnp.zeros((1, 512), jnp.float32)
    for z in reversed(range(64)):
        value = factor_b[pl.ds(z, 1)] - factor_c[pl.ds(z, 1)] * value
        factor_b[pl.ds(z, 1)] = value
    solved = factor_b[...]
    for part in range(4):
        spread[part] = jnp.dot(
            solved,
            x_cosines[:, part * 128 : part * 128 + 128],
            precision=lax.Precision.HIGHEST,
            preferred_element_type=jnp.float32,
        )
    for px, pz in others:
        pltpu.make_async_remote_copy(
            src_ref=spread.at[px, pl.ds(pz, 1)],
            dst_ref=out_rows.at[pl.ds(me, 1)],
            send_sem=send_b,
            recv_sem=recv_b,
            device_id=px * 64 + pz,
            device_id_type=LOGICAL,
        ).start()
    out_rows[pl.ds(me, 1)] = spread[group, pl.ds(layer, 1)]
    pltpu.make_async_copy(rows, rows, send_a).wait()
    pltpu.make_async_copy(rows, rows, send_b).wait()
    pltpu.make_async_copy(rows, rows, recv_b).wait()


def spectral(face_metric, y_rows, x_cosines):
    vmem = pl.BlockSpec(memory_space=pltpu.VMEM)
    return pl.pallas_call(
        spectral_kernel,
        out_shape=jax.ShapeDtypeStruct((256, 128), jnp.float32),
        in_specs=[pl.BlockSpec(memory_space=pltpu.SMEM), vmem, vmem],
        out_specs=vmem,
        scratch_shapes=[
            pltpu.VMEM((4, 64, 128), jnp.float32),
            pltpu.VMEM((4, 64, 128), jnp.float32),
            pltpu.VMEM((64, 512), jnp.float32),
            pltpu.VMEM((64, 512), jnp.float32),
            pltpu.VMEM((64, 512), jnp.float32),
            pltpu.SemaphoreType.DMA,
            pltpu.SemaphoreType.DMA,
            pltpu.SemaphoreType.DMA,
            pltpu.SemaphoreType.DMA,
        ],
        compiler_params=pltpu.CompilerParams(collective_id=0, has_side_effects=True),
    )(face_metric, y_rows, x_cosines)


def per_device(velocity, earlier_term, face_metric):
    z_cells = velocity.shape[1]
    height = velocity.shape[2]
    breadth = velocity.shape[3]
    groups = lax.axis_size("gx")
    length = breadth * groups
    layer_index = lax.axis_index("gz")
    own_faces = lax.dynamic_slice_in_dim(face_metric, layer_index * z_cells, z_cells, 1)
    lower_face = own_faces[0][:, None, None]
    upper_face = own_faces[1][:, None, None]
    metric = 0.5 * (lower_face + upper_face)
    y_cosines = cosine_table(height)
    y_squares = wave_squares(height)
    wide_x = padded(velocity, (("gx", 3),), 1, True)
    wide_z = padded(velocity, (("gz", 1),), 1, False)
    x_after = wide_x[..., 2:]
    x_before = wide_x[..., :-2]
    z_after = wide_z[:, 2:]
    z_before = wide_z[:, :-2]
    y_after, y_before = neighbours_y(velocity)
    grad_x = 0.5 * (x_after - x_before)
    grad_y = 0.5 * (y_after - y_before)
    grad_z = metric * (0.5 * (z_after - z_before))
    lap_x = x_after + x_before - 2.0 * velocity
    lap_z = metric * (upper_face * (z_after - velocity) - lower_face * (velocity - z_before))
    planes = velocity.reshape(3 * z_cells, height, breadth)
    lap_y = inverse_y(y_cosines, -y_squares[:, None] * transform_y(y_cosines, planes)).reshape(
        velocity.shape
    )
    advect = velocity[0:1] * grad_x + velocity[1:2] * grad_y + velocity[2:3] * grad_z
    predicted = velocity + TIME_STEP * (
        -ADVECT_WEIGHT * advect
        + EARLIER_WEIGHT * earlier_term.astype(jnp.float32)
        + VISCOUS_WEIGHT * (lap_x + lap_y + lap_z)
    )
    pred_x = padded(predicted[0], (("gx", 2),), 1, True)
    pred_z = padded(predicted[2], (("gz", 0),), 1, False)
    v_after, v_before = neighbours_y(predicted[1])
    divergence = (
        0.5 * (pred_x[..., 2:] - pred_x[..., :-2])
        + 0.5 * (v_after - v_before)
        + metric * (0.5 * (pred_z[2:] - pred_z[:-2]))
    )
    source = divergence / TIME_STEP
    y_coeffs = transform_y(y_cosines, source)
    spread = spectral(face_metric, y_coeffs[0], cosine_table(length))
    pressure = inverse_y(y_cosines, spread[None])
    wide_p = padded(pressure, (("gx", 2),), 1, True)
    press_x = 0.5 * (wide_p[..., 2:] - wide_p[..., :-2])
    wall_p = padded(pressure, (("gz", 0),), 1, False)
    p_after, p_before = neighbours_y(pressure)
    press_y = 0.5 * (p_after - p_before)
    press_z = metric * (0.5 * (wall_p[2:] - wall_p[:-2]))
    new_velocity = predicted - TIME_STEP * jnp.stack([press_x, press_y, press_z])
    return (new_velocity, pressure)


def solution(mesh):
    placed = (P(None, "gz", None, "gx"), P(None, "gz", None, "gx"), P())
    return jax.shard_map(
        per_device,
        mesh=mesh,
        in_specs=placed,
        out_specs=(P(None, "gz", None, "gx"), P("gz", None, "gx")),
        check_vma=False,
    )
```

```python
import math

import jax
import jax.numpy as jnp
import numpy as np
from jax import lax
from jax.experimental import pallas as pl
from jax.experimental.pallas import tpu as pltpu
from jax.sharding import PartitionSpec as P

TIME_STEP = 0.4
ADVECT_WEIGHT = 5.0 / 12.0
EARLIER_WEIGHT = -17.0 / 60.0
VISCOUS_WEIGHT = 2.0 / 15.0
NX = 512
NY = 256
NZ = 64
LANES = 128
PEERS = 256
LOGICAL = pl.DeviceIdType.LOGICAL
F32 = jnp.float32
BF16 = jnp.bfloat16
NN = (((1,), (0,)), ((), ()))
NT = (((1,), (1,)), ((), ()))
TN = (((0,), (0,)), ((), ()))
Y_SHIFTS = [(i, k, m) for k in (2, 1, 3, 0) for i in (2, 1, 3, 0) for m in (1, 0)]


def cosine_table(extent):
    wavenumber = np.arange(extent)[:, None]
    points = np.arange(extent)[None, :]
    residue = wavenumber * (2 * points + 1) % (4 * extent)
    cosines = np.cos(residue * (math.pi / (2 * extent))) * math.sqrt(2.0 / extent)
    cosines[0] *= math.sqrt(0.5)
    return cosines


def halves(table):
    high = table.astype(np.float32).astype(jnp.bfloat16)
    low = (table - high.astype(np.float64)).astype(np.float32).astype(jnp.bfloat16)
    return np.stack([high, low])


def split(values):
    high = values.astype(BF16)
    low = (values - high.astype(F32)).astype(BF16)
    return high, low


def mul(a, b, dims):
    return lax.dot_general(a, b, dims, preferred_element_type=F32)


def table_times(table, values):
    high, low = split(values)
    t_high, t_low = table[0], table[1]
    return mul(t_high, high, NN) + (mul(t_high, low, NN) + mul(t_low, high, NN))


def times_table(values, table, dims):
    high, low = split(values)
    t_high, t_low = table[0], table[1]
    return mul(high, t_high, dims) + (mul(high, t_low, dims) + mul(low, t_high, dims))


def row_ids(shape):
    return lax.broadcasted_iota(jnp.int32, shape, 0)


def lane_ids(shape):
    return lax.broadcasted_iota(jnp.int32, shape, 1)


def y_neighbours(field):
    rows = row_ids(field.shape)
    count = field.shape[0]
    after = jnp.where(rows == count - 1, field, pltpu.roll(field, count - 1, 0))
    before = jnp.where(rows == 0, field, pltpu.roll(field, 1, 0))
    return after, before


def z_slope(columns, metric):
    rows = row_ids(columns.shape)
    count = columns.shape[0]
    after = jnp.where(rows == count - 1, 0.0, pltpu.roll(columns, count - 1, 0))
    before = jnp.where(rows == 0, 0.0, pltpu.roll(columns, 1, 0))
    return metric * (0.5 * (after - before))


def x_slope(lines):
    count = lines.shape[1]
    return 0.5 * (pltpu.roll(lines, count - 1, 1) - pltpu.roll(lines, 1, 1))


def step_kernel(
    faces,
    velocity,
    earlier,
    y_second,
    y_forward,
    y_inverse,
    x_table,
    new_velocity,
    pressure,
    edges,
    edges_in,
    below,
    above,
    partial,
    y_rows,
    gathered,
    metrics,
    factor_c,
    factor_a,
    factor_b,
    spread,
    returned,
    edge_send,
    edge_recv,
    halo_send,
    halo_recv,
    out_send,
    out_recv,
    back_send,
    back_recv,
):
    group = lax.axis_index("gx")
    layer = lax.axis_index("gz")
    me = group * 64 + layer
    y_parts = [((layer & 6) + (shift << 1)) & 6 for shift in range(4)]
    core_parts = [layer & 1, (layer & 1) ^ 1]
    x_parts = [(group + shift) & 3 for shift in range(4)]

    def each_peer(act):
        def at_shift(shift, combos):
            z_part = ((layer & 56) + (shift << 3)) & 56
            for i, k, m in combos:
                act(x_parts[i], z_part | (y_parts[k] | core_parts[m]))

        def body(j, carry):
            at_shift(4 + (1 - 2 * (j & 1)) * ((j + 1) >> 1), Y_SHIFTS)
            return carry

        lax.fori_loop(0, 7, body, 0)
        at_shift(0, [c for c in Y_SHIFTS if c != (0, 0, 0)])

    barrier = pltpu.get_barrier_semaphore()

    def greet(px, pz):
        pl.semaphore_signal(barrier, inc=1, device_id=px * 64 + pz, device_id_type=LOGICAL)

    each_peer(greet)

    pick_shape = (8, LANES)
    picks = (row_ids(pick_shape) == 0) & (lane_ids(pick_shape) == 0)
    picks |= (row_ids(pick_shape) == 1) & (lane_ids(pick_shape) == LANES - 1)
    picks = picks.astype(F32).astype(BF16)
    for c in range(3):
        high, low = split(velocity[c, 0])
        edges[:, c * NY : c * NY + NY] = mul(picks, high, NT) + mul(picks, low, NT)

    pl.semaphore_wait(barrier, PEERS - 1)

    x_right = ((group + 1) & 3) * 64 + layer
    x_left = ((group + 3) & 3) * 64 + layer
    z_up = group * 64 + ((layer + 1) & 63)
    z_down = group * 64 + ((layer + 63) & 63)

    def remote(source, target, send, recv, peer):
        return pltpu.make_async_remote_copy(
            src_ref=source,
            dst_ref=target,
            send_sem=send,
            recv_sem=recv,
            device_id=peer,
            device_id_type=LOGICAL,
        )

    to_right = remote(edges, edges_in.at[0], edge_send.at[0], edge_recv.at[0], x_right)
    to_left = remote(edges, edges_in.at[1], edge_send.at[1], edge_recv.at[1], x_left)
    to_right.start()
    to_left.start()
    halos = {}
    for c in (0, 2, 1):
        up = remote(velocity.at[c, 0], below.at[c], halo_send.at[0, c], halo_recv.at[0, c], z_up)
        down = remote(velocity.at[c, 0], above.at[c], halo_send.at[1, c], halo_recv.at[1, c], z_down)
        up.start()
        down.start()
        halos[c] = (up, down)

    u = velocity[0, 0]
    v = velocity[1, 0]
    for c in (0, 2, 1):
        field = velocity[c, 0]
        after, before = y_neighbours(field)
        bend = table_times(y_second, field) - 2.0 * field
        partial[c] = field + TIME_STEP * (
            EARLIER_WEIGHT * earlier[c, 0].astype(F32)
            + VISCOUS_WEIGHT * bend
            - ADVECT_WEIGHT * (v * (0.5 * (after - before)))
        )

    k_y = me.astype(F32) * (math.pi / NY)
    k_x = lane_ids((1, NX)).astype(F32) * (math.pi / NX)
    eigen = k_y * k_y + k_x * k_x
    ratio = jnp.zeros((1, NX), F32)
    for z in range(NZ):
        lower = faces[0, z]
        upper = faces[1, z]
        metrics[pl.ds(z, 1)] = jnp.full((1, LANES), 0.5 * (lower + upper), F32)
        per_metric = 2.0 / jnp.full((1, NX), lower + upper, F32)
        inverse = 1.0 / (-(lower + upper) - eigen * per_metric - lower * ratio)
        ratio = upper * inverse
        factor_c[pl.ds(z, 1)] = ratio
        factor_a[pl.ds(z, 1)] = lower * inverse
        factor_b[pl.ds(z, 1)] = (per_metric * inverse) * (1.0 / TIME_STEP)

    to_right.wait()
    to_left.wait()
    place_shape = (16, LANES)
    places = (row_ids(place_shape) == 1) & (lane_ids(place_shape) == 0)
    places |= (row_ids(place_shape) == 8) & (lane_ids(place_shape) == LANES - 1)
    places = places.astype(F32).astype(BF16)
    lanes = lane_ids((NY, LANES))
    for c in (0, 2, 1):
        field = velocity[c, 0]
        part = slice(c * NY, c * NY + NY)
        high, low = split(jnp.concatenate([edges_in[0, :, part], edges_in[1, :, part]], 0))
        outer = mul(high, places, TN) + mul(low, places, TN)
        after = jnp.where(lanes == LANES - 1, outer, pltpu.roll(field, LANES - 1, 1))
        before = jnp.where(lanes == 0, outer, pltpu.roll(field, 1, 1))
        partial[c] = partial[c] + TIME_STEP * (
            VISCOUS_WEIGHT * (after + before) - ADVECT_WEIGHT * (u * (0.5 * (after - before)))
        )

    lower = faces[0, layer]
    upper = faces[1, layer]
    metric = 0.5 * (lower + upper)
    w = velocity[2, 0]
    for c in (0, 2, 1):
        for copy in halos[c]:
            copy.wait()
        field = velocity[c, 0]
        after = jnp.where(layer == NZ - 1, 0.0, above[c])
        before = jnp.where(layer == 0, 0.0, below[c])
        bend = metric * (upper * (after - field) - lower * (field - before))
        predicted = partial[c] + TIME_STEP * (
            VISCOUS_WEIGHT * bend - ADVECT_WEIGHT * (w * (metric * (0.5 * (after - before))))
        )
        partial[c] = predicted
        if c == 1:
            after, before = y_neighbours(predicted)
            predicted = 0.5 * (after - before)
        y_rows[c] = table_times(y_forward, predicted)

        def send(px, pz):
            peer = px * 64 + pz
            remote(
                y_rows.at[c, pl.ds(peer, 1)],
                gathered.at[c, group, pl.ds(layer, 1)],
                out_send.at[c],
                out_recv.at[c],
                peer,
            ).start()

        each_peer(send)
        gathered[c, group, pl.ds(layer, 1)] = y_rows[c, pl.ds(me, 1)]

    others = returned.at[0, pl.ds(0, PEERS - 1)]

    def finish(sem):
        pltpu.make_async_copy(others, others, sem).wait()

    def lines(c):
        return jnp.concatenate([gathered[c, part] for part in range(4)], 1)

    metric_rows = jnp.concatenate([metrics[...]] * 4, 1)
    finish(out_recv.at[0])
    source = x_slope(lines(0))
    finish(out_recv.at[2])
    source = source + z_slope(lines(2), metric_rows)
    finish(out_recv.at[1])
    source = source + lines(1)
    factor_b[...] = factor_b[...] * times_table(source, x_table, NT)
    value = jnp.zeros((1, NX), F32)
    for z in range(NZ):
        value = factor_b[pl.ds(z, 1)] - factor_a[pl.ds(z, 1)] * value
        factor_b[pl.ds(z, 1)] = value
    value = jnp.zeros((1, NX), F32)
    for z in reversed(range(NZ)):
        value = factor_b[pl.ds(z, 1)] - factor_c[pl.ds(z, 1)] * value
        factor_b[pl.ds(z, 1)] = value
    solved = times_table(factor_b[...], x_table, NN)
    for c, lined in ((1, solved), (0, x_slope(solved)), (2, z_slope(solved, metric_rows))):
        for part in range(4):
            spread[c, part] = lined[:, part * LANES : part * LANES + LANES]

        def send_back(px, pz):
            remote(
                spread.at[c, px, pl.ds(pz, 1)],
                returned.at[c, pl.ds(me, 1)],
                back_send.at[c],
                back_recv.at[c],
                px * 64 + pz,
            ).start()

        each_peer(send_back)
        returned[c, pl.ds(me, 1)] = spread[c, group, pl.ds(layer, 1)]

    for c in (1, 0, 2):
        finish(back_recv.at[c])
        field = table_times(y_inverse, returned[c])
        if c == 1:
            pressure[0] = field
            after, before = y_neighbours(field)
            field = 0.5 * (after - before)
        new_velocity[c, 0] = partial[c] - TIME_STEP * field
    for c in range(3):
        finish(out_send.at[c])
        finish(back_send.at[c])


def per_device(velocity, earlier_term, face_metric):
    y_cosines = cosine_table(NY)
    y_squares = (np.arange(NY) * (math.pi / NY)) ** 2
    y_second = -(y_cosines.T * y_squares) @ y_cosines
    vmem = pl.BlockSpec(memory_space=pltpu.VMEM)
    dma = pltpu.SemaphoreType.DMA
    return pl.pallas_call(
        step_kernel,
        out_shape=(
            jax.ShapeDtypeStruct(velocity.shape, F32),
            jax.ShapeDtypeStruct(velocity.shape[1:], F32),
        ),
        in_specs=[pl.BlockSpec(memory_space=pltpu.SMEM)] + [vmem] * 6,
        out_specs=(vmem, vmem),
        scratch_shapes=[
            pltpu.VMEM((8, 3 * NY), F32),
            pltpu.VMEM((2, 8, 3 * NY), F32),
            pltpu.VMEM((3, NY, LANES), F32),
            pltpu.VMEM((3, NY, LANES), F32),
            pltpu.VMEM((3, NY, LANES), F32),
            pltpu.VMEM((3, NY, LANES), F32),
            pltpu.VMEM((3, 4, NZ, LANES), F32),
            pltpu.VMEM((NZ, LANES), F32),
            pltpu.VMEM((NZ, NX), F32),
            pltpu.VMEM((NZ, NX), F32),
            pltpu.VMEM((NZ, NX), F32),
            pltpu.VMEM((3, 4, NZ, LANES), F32),
            pltpu.VMEM((3, NY, LANES), F32),
            dma((2,)),
            dma((2,)),
            dma((2, 3)),
            dma((2, 3)),
            dma((3,)),
            dma((3,)),
            dma((3,)),
            dma((3,)),
        ],
        compiler_params=pltpu.CompilerParams(collective_id=0, has_side_effects=True),
    )(
        face_metric,
        velocity,
        earlier_term,
        jnp.asarray(halves(y_second)),
        jnp.asarray(halves(y_cosines)),
        jnp.asarray(halves(y_cosines.T)),
        jnp.asarray(halves(cosine_table(NX))),
    )


def solution(mesh):
    placed = (P(None, "gz", None, "gx"), P(None, "gz", None, "gx"), P())
    return jax.shard_map(
        per_device,
        mesh=mesh,
        in_specs=placed,
        out_specs=(P(None, "gz", None, "gx"), P("gz", None, "gx")),
        check_vma=False,
    )
```

```python
import math

import jax
import jax.numpy as jnp
import numpy as np
from jax import lax
from jax.experimental import pallas as pl
from jax.experimental.pallas import tpu as pltpu
from jax.sharding import PartitionSpec as P

TIME_STEP = 0.4
ADVECT_WEIGHT = 5.0 / 12.0
EARLIER_WEIGHT = -17.0 / 60.0
VISCOUS_WEIGHT = 2.0 / 15.0
NX = 512
NY = 256
NZ = 64
LANES = 128
PEERS = 256
LOGICAL = pl.DeviceIdType.LOGICAL
F32 = jnp.float32
BF16 = jnp.bfloat16
NN = (((1,), (0,)), ((), ()))
NT = (((1,), (1,)), ((), ()))
TN = (((0,), (0,)), ((), ()))
Y_SHIFTS = [(i, k, m) for k in (2, 1, 3, 0) for i in (2, 1, 3, 0) for m in (1, 0)]


def cosine_table(extent):
    wavenumber = np.arange(extent)[:, None]
    points = np.arange(extent)[None, :]
    residue = wavenumber * (2 * points + 1) % (4 * extent)
    cosines = np.cos(residue * (math.pi / (2 * extent))) * math.sqrt(2.0 / extent)
    cosines[0] *= math.sqrt(0.5)
    return cosines


def halves(table):
    high = table.astype(np.float32).astype(jnp.bfloat16)
    low = (table - high.astype(np.float64)).astype(np.float32).astype(jnp.bfloat16)
    return np.stack([high, low])


def split(values):
    high = values.astype(BF16)
    low = (values - high.astype(F32)).astype(BF16)
    return high, low


def mul(a, b, dims):
    return lax.dot_general(a, b, dims, preferred_element_type=F32)


def table_times(table, values):
    high, low = split(values)
    t_high, t_low = table[0], table[1]
    return mul(t_high, high, NN) + (mul(t_high, low, NN) + mul(t_low, high, NN))


def times_table(values, table, dims):
    high, low = split(values)
    t_high, t_low = table[0], table[1]
    return mul(high, t_high, dims) + (mul(high, t_low, dims) + mul(low, t_high, dims))


def row_ids(shape):
    return lax.broadcasted_iota(jnp.int32, shape, 0)


def lane_ids(shape):
    return lax.broadcasted_iota(jnp.int32, shape, 1)


def y_neighbours(field):
    rows = row_ids(field.shape)
    count = field.shape[0]
    after = jnp.where(rows == count - 1, field, pltpu.roll(field, count - 1, 0))
    before = jnp.where(rows == 0, field, pltpu.roll(field, 1, 0))
    return after, before


def z_slope(columns, metric):
    rows = row_ids(columns.shape)
    count = columns.shape[0]
    after = jnp.where(rows == count - 1, 0.0, pltpu.roll(columns, count - 1, 0))
    before = jnp.where(rows == 0, 0.0, pltpu.roll(columns, 1, 0))
    return metric * (0.5 * (after - before))


def x_slope(lines):
    count = lines.shape[1]
    return 0.5 * (pltpu.roll(lines, count - 1, 1) - pltpu.roll(lines, 1, 1))


def lined_x(field, edge_rows):
    shape = (16, LANES)
    places = (row_ids(shape) == 1) & (lane_ids(shape) == 0)
    places |= (row_ids(shape) == 8) & (lane_ids(shape) == LANES - 1)
    places = places.astype(F32).astype(BF16)
    high, low = split(edge_rows)
    outer = mul(high, places, TN) + mul(low, places, TN)
    lanes = lane_ids(field.shape)
    after = jnp.where(lanes == LANES - 1, outer, pltpu.roll(field, LANES - 1, 1))
    before = jnp.where(lanes == 0, outer, pltpu.roll(field, 1, 1))
    return after, before


def edge_lines(field):
    shape = (8, LANES)
    picks = (row_ids(shape) == 0) & (lane_ids(shape) == 0)
    picks |= (row_ids(shape) == 1) & (lane_ids(shape) == LANES - 1)
    picks = picks.astype(F32).astype(BF16)
    high, low = split(field)
    return mul(picks, high, NT) + mul(picks, low, NT)


def step_kernel(
    faces,
    velocity_in,
    earlier_in,
    y_second_in,
    y_forward_in,
    y_inverse_in,
    x_table_in,
    new_velocity,
    pressure,
    velocity,
    earlier,
    y_second,
    y_forward,
    y_inverse,
    x_table,
    edges,
    edges_in,
    below,
    above,
    partial,
    y_rows,
    gathered,
    metrics,
    factor_c,
    factor_a,
    factor_b,
    spread,
    returned,
    load_sem,
    edge_send,
    edge_recv,
    halo_send,
    halo_recv,
    out_send,
    out_recv,
    back_send,
    back_recv,
    plane_token,
    line_token,
):
    loads = [
        pltpu.make_async_copy(source, target, load_sem.at[i])
        for i, (source, target) in enumerate(
            (
                (velocity_in, velocity),
                (y_second_in, y_second),
                (earlier_in, earlier),
                (y_forward_in, y_forward),
                (x_table_in, x_table),
                (y_inverse_in, y_inverse),
            )
        )
    ]
    for load in loads:
        load.start()

    group = lax.axis_index("gx")
    layer = lax.axis_index("gz")
    me = group * 64 + layer
    y_parts = [((layer & 6) + (shift << 1)) & 6 for shift in range(4)]
    core_parts = [layer & 1, (layer & 1) ^ 1]
    x_parts = [(group + shift) & 3 for shift in range(4)]
    x_line = [x_parts[i] * 64 + layer for i in (1, 3, 2)]
    y_line = [
        group * 64 + ((layer & 56) | (y_parts[k] | core_parts[m]))
        for k, m in ((0, 1), (1, 0), (1, 1), (3, 0), (3, 1), (2, 0), (2, 1))
    ]
    z_line = [
        group * 64 + (((layer & 56) + (shift << 3)) & 56) + (layer & 7)
        for shift in (1, 7, 2, 6, 3, 5, 4)
    ]
    x_right, x_left = x_line[0], x_line[1]
    z_up = group * 64 + ((layer + 1) & 63)
    z_down = group * 64 + ((layer + 63) & 63)
    at_top = (layer & 7) == 7
    at_bottom = (layer & 7) == 0

    def tell(sem, peer):
        pl.semaphore_signal(sem, inc=1, device_id=peer, device_id_type=LOGICAL)

    def each_peer(act):
        def at_shift(shift, combos):
            z_part = ((layer & 56) + (shift << 3)) & 56
            for i, k, m in combos:
                act(x_parts[i], z_part | (y_parts[k] | core_parts[m]))

        def body(j, carry):
            at_shift(4 + (1 - 2 * (j & 1)) * ((j + 1) >> 1), Y_SHIFTS)
            return carry

        lax.fori_loop(0, 7, body, 0)
        at_shift(0, [c for c in Y_SHIFTS if c != (0, 0, 0)])

    def remote(source, target, send, recv, peer):
        return pltpu.make_async_remote_copy(
            src_ref=source,
            dst_ref=target,
            send_sem=send,
            recv_sem=recv,
            device_id=peer,
            device_id_type=LOGICAL,
        )

    barrier = pltpu.get_barrier_semaphore()

    @pl.when(at_top)
    def _():
        tell(barrier, z_up)

    @pl.when(at_bottom)
    def _():
        tell(barrier, z_down)

    for peer in y_line + x_line + z_line:
        tell(barrier, peer)
    loads[0].wait()
    for c in range(3):
        edges[0, :, c * NY : c * NY + NY] = edge_lines(velocity[c, 0])
    pl.semaphore_wait(
        barrier, 17 + jnp.where(at_top, 1, 0) + jnp.where(at_bottom, 1, 0)
    )

    halos = {}
    for c in (0, 2, 1):
        up = remote(velocity.at[c, 0], below.at[c], halo_send.at[0, c], halo_recv.at[0, c], z_up)
        down = remote(velocity.at[c, 0], above.at[c], halo_send.at[1, c], halo_recv.at[1, c], z_down)
        up.start()
        down.start()
        halos[c] = (up, down)

    def send_edges(k, width):
        copies = []
        for side, peer in enumerate((x_right, x_left)):
            copies.append(
                remote(
                    edges.at[k, :, pl.ds(0, width)],
                    edges_in.at[k, side, :, pl.ds(0, width)],
                    edge_send.at[k, side],
                    edge_recv.at[k, side],
                    peer,
                )
            )
            copies[-1].start()
        return copies

    def edge_pair(k, first):
        part = slice(first, first + NY)
        return jnp.concatenate([edges_in[k, 0, :, part], edges_in[k, 1, :, part]], 0)

    velocity_edges = send_edges(0, 3 * NY)
    for peer in y_line:
        tell(plane_token, peer)

    u = velocity[0, 0]
    v = velocity[1, 0]
    loads[1].wait()
    loads[2].wait()
    for c in (0, 2, 1):
        field = velocity[c, 0]
        after, before = y_neighbours(field)
        bend = table_times(y_second, field) - 2.0 * field
        partial[c] = field + TIME_STEP * (
            EARLIER_WEIGHT * earlier[c, 0].astype(F32)
            + VISCOUS_WEIGHT * bend
            - ADVECT_WEIGHT * (v * (0.5 * (after - before)))
        )

    pl.semaphore_wait(plane_token, 7)
    for peer in x_line:
        tell(line_token, peer)

    for copy in velocity_edges:
        copy.wait()
    for c in (0, 2, 1):
        after, before = lined_x(velocity[c, 0], edge_pair(0, c * NY))
        partial[c] = partial[c] + TIME_STEP * (
            VISCOUS_WEIGHT * (after + before) - ADVECT_WEIGHT * (u * (0.5 * (after - before)))
        )
    loads[3].wait()

    lower = faces[0, layer]
    upper = faces[1, layer]
    metric = 0.5 * (lower + upper)
    w = velocity[2, 0]

    def predict(c):
        for copy in halos[c]:
            copy.wait()
        field = velocity[c, 0]
        after = jnp.where(layer == NZ - 1, 0.0, above[c])
        before = jnp.where(layer == 0, 0.0, below[c])
        bend = metric * (upper * (after - field) - lower * (field - before))
        predicted = partial[c] + TIME_STEP * (
            VISCOUS_WEIGHT * bend - ADVECT_WEIGHT * (w * (metric * (0.5 * (after - before))))
        )
        partial[c] = predicted
        return predicted

    def send_rows(slot, field):
        y_rows[slot] = table_times(y_forward, field)

        def send(px, pz):
            peer = px * 64 + pz
            remote(
                y_rows.at[slot, pl.ds(peer, 1)],
                gathered.at[slot, group, pl.ds(layer, 1)],
                out_send.at[slot],
                out_recv.at[slot],
                peer,
            ).start()

        each_peer(send)
        gathered[slot, group, pl.ds(layer, 1)] = y_rows[slot, pl.ds(me, 1)]

    predicted_u = predict(0)
    edges[1, :, :NY] = edge_lines(predicted_u)
    u_edges = send_edges(1, NY)
    predicted_w = predict(2)
    pl.semaphore_wait(line_token, 3)
    send_rows(0, predicted_w)
    after, before = y_neighbours(predict(1))
    flow = after - before
    for copy in u_edges:
        copy.wait()
    after, before = lined_x(partial[0], edge_pair(1, 0))
    send_rows(1, 0.5 * (flow + (after - before)))

    k_y = me.astype(F32) * (math.pi / NY)
    k_x = lane_ids((1, NX)).astype(F32) * (math.pi / NX)
    eigen = k_y * k_y + k_x * k_x
    ratio = jnp.zeros((1, NX), F32)
    for z in range(NZ):
        lower = faces[0, z]
        upper = faces[1, z]
        metrics[pl.ds(z, 1)] = jnp.full((1, LANES), 0.5 * (lower + upper), F32)
        per_metric = 2.0 / jnp.full((1, NX), lower + upper, F32)
        inverse = 1.0 / (-(lower + upper) - eigen * per_metric - lower * ratio)
        ratio = upper * inverse
        factor_c[pl.ds(z, 1)] = ratio
        factor_a[pl.ds(z, 1)] = lower * inverse
        factor_b[pl.ds(z, 1)] = (per_metric * inverse) * (1.0 / TIME_STEP)
    metric_rows = jnp.concatenate([metrics[...]] * 4, 1)
    loads[4].wait()
    loads[5].wait()

    others = returned.at[0, pl.ds(0, PEERS - 1)]

    def finish(sem):
        pltpu.make_async_copy(others, others, sem).wait()

    def lines(slot):
        return jnp.concatenate([gathered[slot, part] for part in range(4)], 1)

    finish(out_recv.at[0])
    source = z_slope(lines(0), metric_rows)
    finish(out_recv.at[1])
    source = source + lines(1)
    factor_b[...] = factor_b[...] * times_table(source, x_table, NT)
    value = jnp.zeros((1, NX), F32)
    for z in range(NZ):
        value = factor_b[pl.ds(z, 1)] - factor_a[pl.ds(z, 1)] * value
        factor_b[pl.ds(z, 1)] = value
    value = jnp.zeros((1, NX), F32)
    for z in reversed(range(NZ)):
        value = factor_b[pl.ds(z, 1)] - factor_c[pl.ds(z, 1)] * value
        factor_b[pl.ds(z, 1)] = value
    solved = times_table(factor_b[...], x_table, NN)
    for slot, lined in ((0, solved), (1, z_slope(solved, metric_rows))):
        for part in range(4):
            spread[slot, part] = lined[:, part * LANES : part * LANES + LANES]

        def send_back(px, pz):
            remote(
                spread.at[slot, px, pl.ds(pz, 1)],
                returned.at[slot, pl.ds(me, 1)],
                back_send.at[slot],
                back_recv.at[slot],
                px * 64 + pz,
            ).start()

        each_peer(send_back)
        returned[slot, pl.ds(me, 1)] = spread[slot, group, pl.ds(layer, 1)]

    finish(back_recv.at[0])
    rows = returned[0]
    edges[2, :, :NY] = edge_lines(rows)
    p_edges = send_edges(2, NY)
    field = table_times(y_inverse, rows)
    pressure[0] = field
    after, before = y_neighbours(field)
    new_velocity[1, 0] = partial[1] - (0.5 * TIME_STEP) * (after - before)
    for copy in p_edges:
        copy.wait()
    after, before = lined_x(rows, edge_pair(2, 0))
    new_velocity[0, 0] = partial[0] - TIME_STEP * table_times(y_inverse, 0.5 * (after - before))
    finish(back_recv.at[1])
    new_velocity[2, 0] = partial[2] - TIME_STEP * table_times(y_inverse, returned[1])
    for slot in range(2):
        finish(out_send.at[slot])
        finish(back_send.at[slot])


def per_device(velocity, earlier_term, face_metric):
    y_cosines = cosine_table(NY)
    y_squares = (np.arange(NY) * (math.pi / NY)) ** 2
    y_second = -(y_cosines.T * y_squares) @ y_cosines
    vmem = pl.BlockSpec(memory_space=pltpu.VMEM)
    hbm = pl.BlockSpec(memory_space=pltpu.HBM)
    dma = pltpu.SemaphoreType.DMA
    return pl.pallas_call(
        step_kernel,
        out_shape=(
            jax.ShapeDtypeStruct(velocity.shape, F32),
            jax.ShapeDtypeStruct(velocity.shape[1:], F32),
        ),
        in_specs=[pl.BlockSpec(memory_space=pltpu.SMEM)] + [hbm] * 6,
        out_specs=(vmem, vmem),
        scratch_shapes=[
            pltpu.VMEM((3, 1, NY, LANES), F32),
            pltpu.VMEM((3, 1, NY, LANES), BF16),
            pltpu.VMEM((2, NY, NY), BF16),
            pltpu.VMEM((2, NY, NY), BF16),
            pltpu.VMEM((2, NY, NY), BF16),
            pltpu.VMEM((2, NX, NX), BF16),
            pltpu.VMEM((3, 8, 3 * NY), F32),
            pltpu.VMEM((3, 2, 8, 3 * NY), F32),
            pltpu.VMEM((3, NY, LANES), F32),
            pltpu.VMEM((3, NY, LANES), F32),
            pltpu.VMEM((3, NY, LANES), F32),
            pltpu.VMEM((2, NY, LANES), F32),
            pltpu.VMEM((2, 4, NZ, LANES), F32),
            pltpu.VMEM((NZ, LANES), F32),
            pltpu.VMEM((NZ, NX), F32),
            pltpu.VMEM((NZ, NX), F32),
            pltpu.VMEM((NZ, NX), F32),
            pltpu.VMEM((2, 4, NZ, LANES), F32),
            pltpu.VMEM((2, NY, LANES), F32),
            dma((6,)),
            dma((3, 2)),
            dma((3, 2)),
            dma((2, 3)),
            dma((2, 3)),
            dma((2,)),
            dma((2,)),
            dma((2,)),
            dma((2,)),
            pltpu.SemaphoreType.REGULAR,
            pltpu.SemaphoreType.REGULAR,
        ],
        compiler_params=pltpu.CompilerParams(
            collective_id=0, has_side_effects=True
        ),
    )(
        face_metric,
        velocity,
        earlier_term,
        jnp.asarray(halves(y_second)),
        jnp.asarray(halves(y_cosines)),
        jnp.asarray(halves(y_cosines.T)),
        jnp.asarray(halves(cosine_table(NX))),
    )


def solution(mesh):
    placed = (P(None, "gz", None, "gx"), P(None, "gz", None, "gx"), P())
    return jax.shard_map(
        per_device,
        mesh=mesh,
        in_specs=placed,
        out_specs=(P(None, "gz", None, "gx"), P("gz", None, "gx")),
        check_vma=False,
    )
```

```python
import math

import jax
import jax.numpy as jnp
import numpy as np
from jax import lax
from jax.experimental import pallas as pl
from jax.experimental.pallas import tpu as pltpu
from jax.sharding import PartitionSpec as P

TIME_STEP = 0.4
ADVECT_WEIGHT = 5.0 / 12.0
EARLIER_WEIGHT = -17.0 / 60.0
VISCOUS_WEIGHT = 2.0 / 15.0
NX = 512
NY = 256
NZ = 64
LANES = 128
PEERS = 256
LOGICAL = pl.DeviceIdType.LOGICAL
F32 = jnp.float32
BF16 = jnp.bfloat16
NN = (((1,), (0,)), ((), ()))
NT = (((1,), (1,)), ((), ()))
TN = (((0,), (0,)), ((), ()))
Y_SHIFTS = [(i, k, m) for k in (2, 1, 3, 0) for i in (2, 1, 3, 0) for m in (1, 0)]


def cosine_table(extent):
    wavenumber = np.arange(extent)[:, None]
    points = np.arange(extent)[None, :]
    residue = wavenumber * (2 * points + 1) % (4 * extent)
    cosines = np.cos(residue * (math.pi / (2 * extent))) * math.sqrt(2.0 / extent)
    cosines[0] *= math.sqrt(0.5)
    return cosines


def halves(table):
    high = table.astype(np.float32).astype(jnp.bfloat16)
    low = (table - high.astype(np.float64)).astype(np.float32).astype(jnp.bfloat16)
    return np.stack([high, low])


def split(values):
    high = values.astype(BF16)
    low = (values - high.astype(F32)).astype(BF16)
    return high, low


def mul(a, b, dims):
    return lax.dot_general(a, b, dims, preferred_element_type=F32)


def table_times(table, values):
    high, low = split(values)
    t_high, t_low = table[0], table[1]
    return mul(t_high, high, NN) + (mul(t_high, low, NN) + mul(t_low, high, NN))


def times_table(values, table, dims):
    high, low = split(values)
    t_high, t_low = table[0], table[1]
    return mul(high, t_high, dims) + (mul(high, t_low, dims) + mul(low, t_high, dims))


def row_ids(shape):
    return lax.broadcasted_iota(jnp.int32, shape, 0)


def lane_ids(shape):
    return lax.broadcasted_iota(jnp.int32, shape, 1)


def y_neighbours(field):
    rows = row_ids(field.shape)
    count = field.shape[0]
    after = jnp.where(rows == count - 1, field, pltpu.roll(field, count - 1, 0))
    before = jnp.where(rows == 0, field, pltpu.roll(field, 1, 0))
    return after, before


def z_slope(columns, metric):
    rows = row_ids(columns.shape)
    count = columns.shape[0]
    after = jnp.where(rows == count - 1, 0.0, pltpu.roll(columns, count - 1, 0))
    before = jnp.where(rows == 0, 0.0, pltpu.roll(columns, 1, 0))
    return metric * (0.5 * (after - before))


def x_slope(lines):
    count = lines.shape[1]
    return 0.5 * (pltpu.roll(lines, count - 1, 1) - pltpu.roll(lines, 1, 1))


def lined_x(field, edge_rows):
    shape = (16, LANES)
    places = (row_ids(shape) == 1) & (lane_ids(shape) == 0)
    places |= (row_ids(shape) == 8) & (lane_ids(shape) == LANES - 1)
    places = places.astype(F32).astype(BF16)
    high, low = split(edge_rows)
    outer = mul(high, places, TN) + mul(low, places, TN)
    lanes = lane_ids(field.shape)
    after = jnp.where(lanes == LANES - 1, outer, pltpu.roll(field, LANES - 1, 1))
    before = jnp.where(lanes == 0, outer, pltpu.roll(field, 1, 1))
    return after, before


def edge_lines(field):
    shape = (8, LANES)
    picks = (row_ids(shape) == 0) & (lane_ids(shape) == 0)
    picks |= (row_ids(shape) == 1) & (lane_ids(shape) == LANES - 1)
    picks = picks.astype(F32).astype(BF16)
    high, low = split(field)
    return mul(picks, high, NT) + mul(picks, low, NT)


def step_kernel(
    faces,
    velocity_in,
    earlier_in,
    y_second_in,
    y_forward_in,
    y_inverse_in,
    x_table_in,
    new_velocity,
    pressure,
    velocity,
    earlier,
    y_second,
    y_forward,
    y_inverse,
    x_table,
    edges,
    edges_in,
    edges_z,
    below,
    above,
    partial,
    y_rows,
    gathered,
    metrics,
    factor_c,
    factor_a,
    factor_b,
    spread,
    returned,
    load_sem,
    edge_send,
    edge_recv,
    halo_send,
    halo_recv,
    out_send,
    out_recv,
    back_send,
    back_recv,
    plane_token,
    line_token,
):
    loads = [
        pltpu.make_async_copy(source, target, load_sem.at[i])
        for i, (source, target) in enumerate(
            (
                (velocity_in.at[0], velocity.at[0]),
                (velocity_in.at[2], velocity.at[2]),
                (velocity_in.at[1], velocity.at[1]),
                (y_second_in, y_second),
                (earlier_in, earlier),
                (y_forward_in, y_forward),
                (x_table_in, x_table),
                (y_inverse_in, y_inverse),
            )
        )
    ]
    for load in loads:
        load.start()

    group = lax.axis_index("gx")
    layer = lax.axis_index("gz")
    me = group * 64 + layer
    y_parts = [((layer & 6) + (shift << 1)) & 6 for shift in range(4)]
    core_parts = [layer & 1, (layer & 1) ^ 1]
    x_parts = [(group + shift) & 3 for shift in range(4)]
    x_line = [x_parts[i] * 64 + layer for i in (1, 3, 2)]
    y_line = [
        group * 64 + ((layer & 56) | (y_parts[k] | core_parts[m]))
        for k, m in ((0, 1), (1, 0), (1, 1), (3, 0), (3, 1), (2, 0), (2, 1))
    ]
    z_line = [
        group * 64 + (((layer & 56) + (shift << 3)) & 56) + (layer & 7)
        for shift in (1, 7, 2, 6, 3, 5, 4)
    ]
    x_right, x_left = x_line[0], x_line[1]
    z_up = group * 64 + ((layer + 1) & 63)
    z_down = group * 64 + ((layer + 63) & 63)
    at_top = (layer & 7) == 7
    at_bottom = (layer & 7) == 0

    def tell(sem, peer):
        pl.semaphore_signal(sem, inc=1, device_id=peer, device_id_type=LOGICAL)

    def each_peer(act):
        def at_shift(shift, combos):
            z_part = ((layer & 56) + (shift << 3)) & 56
            for i, k, m in combos:
                act(x_parts[i], z_part | (y_parts[k] | core_parts[m]))

        def body(j, carry):
            at_shift(4 + (1 - 2 * (j & 1)) * ((j + 1) >> 1), Y_SHIFTS)
            return carry

        lax.fori_loop(0, 7, body, 0)
        at_shift(0, [c for c in Y_SHIFTS if c != (0, 0, 0)])

    def remote(source, target, send, recv, peer):
        return pltpu.make_async_remote_copy(
            src_ref=source,
            dst_ref=target,
            send_sem=send,
            recv_sem=recv,
            device_id=peer,
            device_id_type=LOGICAL,
        )

    barrier = pltpu.get_barrier_semaphore()

    @pl.when(at_top)
    def _():
        tell(barrier, z_up)

    @pl.when(at_bottom)
    def _():
        tell(barrier, z_down)

    for peer in y_line + x_line + z_line:
        tell(barrier, peer)
    for i in range(3):
        loads[i].wait()
    for c in range(3):
        edges[0, :, c * NY : c * NY + NY] = edge_lines(velocity[c, 0])
    pl.semaphore_wait(
        barrier, 17 + jnp.where(at_top, 1, 0) + jnp.where(at_bottom, 1, 0)
    )

    def send_edges(k, width):
        copies = []
        for side, peer in enumerate((x_right, x_left)):
            copies.append(
                remote(
                    edges.at[k, :, pl.ds(0, width)],
                    edges_in.at[k, side, :, pl.ds(0, width)],
                    edge_send.at[k, side],
                    edge_recv.at[k, side],
                    peer,
                )
            )
            copies[-1].start()
        return copies

    def edge_pair(k, first):
        part = slice(first, first + NY)
        return jnp.concatenate([edges_in[k, 0, :, part], edges_in[k, 1, :, part]], 0)

    velocity_edges = send_edges(0, 3 * NY)
    layer_edges = []
    for side, peer in enumerate((z_up, z_down)):
        layer_edges.append(
            remote(
                edges.at[0], edges_z.at[side], edge_send.at[3, side], edge_recv.at[3, side], peer
            )
        )
        layer_edges[-1].start()
    halos = {}
    for c in (2, 0, 1):
        up = remote(velocity.at[c, 0], below.at[c], halo_send.at[0, c], halo_recv.at[0, c], z_up)
        down = remote(velocity.at[c, 0], above.at[c], halo_send.at[1, c], halo_recv.at[1, c], z_down)
        up.start()
        down.start()
        halos[c] = (up, down)
    for peer in y_line:
        tell(plane_token, peer)

    u = velocity[0, 0]
    v = velocity[1, 0]
    loads[3].wait()
    loads[4].wait()
    for c in (0, 2, 1):
        field = velocity[c, 0]
        after, before = y_neighbours(field)
        bend = table_times(y_second, field) - 2.0 * field
        partial[c] = field + TIME_STEP * (
            EARLIER_WEIGHT * earlier[c, 0].astype(F32)
            + VISCOUS_WEIGHT * bend
            - ADVECT_WEIGHT * (v * (0.5 * (after - before)))
        )

    pl.semaphore_wait(plane_token, 7)
    for peer in x_line:
        tell(line_token, peer)

    lower = faces[0, layer]
    upper = faces[1, layer]
    metric = 0.5 * (lower + upper)
    w = velocity[2, 0]

    def with_z(base, field, below_it, above_it, drift):
        after = jnp.where(layer == NZ - 1, 0.0, above_it)
        before = jnp.where(layer == 0, 0.0, below_it)
        bend = metric * (upper * (after - field) - lower * (field - before))
        return base + TIME_STEP * (
            VISCOUS_WEIGHT * bend - ADVECT_WEIGHT * (drift * (metric * (0.5 * (after - before))))
        )

    def add_x(c):
        after, before = lined_x(velocity[c, 0], edge_pair(0, c * NY))
        partial[c] = partial[c] + TIME_STEP * (
            VISCOUS_WEIGHT * (after + before) - ADVECT_WEIGHT * (u * (0.5 * (after - before)))
        )

    def predict(c):
        for copy in halos[c]:
            copy.wait()
        predicted = with_z(partial[c], velocity[c, 0], below[c], above[c], w)
        partial[c] = predicted
        return predicted

    for copy in velocity_edges:
        copy.wait()
    add_x(0)
    own = edge_lines(partial[0])
    for copy in layer_edges:
        copy.wait()
    edges[1, :, :NY] = with_z(
        own,
        edges[0, :, :NY],
        edges_z[0, :, :NY],
        edges_z[1, :, :NY],
        edges[0, :, 2 * NY :],
    )
    u_edges = send_edges(1, NY)
    add_x(2)
    add_x(1)
    loads[5].wait()

    def send_rows(slot, field):
        y_rows[slot] = table_times(y_forward, field)

        def send(px, pz):
            peer = px * 64 + pz
            remote(
                y_rows.at[slot, pl.ds(peer, 1)],
                gathered.at[slot, group, pl.ds(layer, 1)],
                out_send.at[slot],
                out_recv.at[slot],
                peer,
            ).start()

        each_peer(send)
        gathered[slot, group, pl.ds(layer, 1)] = y_rows[slot, pl.ds(me, 1)]

    predicted_w = predict(2)
    pl.semaphore_wait(line_token, 3)
    send_rows(0, predicted_w)
    predicted_u = predict(0)
    for copy in u_edges:
        copy.wait()
    after, before = lined_x(predicted_u, edge_pair(1, 0))
    flow = after - before
    after, before = y_neighbours(predict(1))
    send_rows(1, 0.5 * (flow + (after - before)))

    k_y = me.astype(F32) * (math.pi / NY)
    k_x = lane_ids((1, NX)).astype(F32) * (math.pi / NX)
    eigen = k_y * k_y + k_x * k_x
    ratio = jnp.zeros((1, NX), F32)
    for z in range(NZ):
        lower = faces[0, z]
        upper = faces[1, z]
        metrics[pl.ds(z, 1)] = jnp.full((1, LANES), 0.5 * (lower + upper), F32)
        per_metric = 2.0 / jnp.full((1, NX), lower + upper, F32)
        inverse = 1.0 / (-(lower + upper) - eigen * per_metric - lower * ratio)
        ratio = upper * inverse
        factor_c[pl.ds(z, 1)] = ratio
        factor_a[pl.ds(z, 1)] = lower * inverse
        factor_b[pl.ds(z, 1)] = (per_metric * inverse) * (1.0 / TIME_STEP)
    metric_rows = jnp.concatenate([metrics[...]] * 4, 1)
    loads[6].wait()
    loads[7].wait()

    others = returned.at[0, pl.ds(0, PEERS - 1)]

    def finish(sem):
        pltpu.make_async_copy(others, others, sem).wait()

    def lines(slot):
        return jnp.concatenate([gathered[slot, part] for part in range(4)], 1)

    finish(out_recv.at[0])
    source = z_slope(lines(0), metric_rows)
    finish(out_recv.at[1])
    source = source + lines(1)
    factor_b[...] = factor_b[...] * times_table(source, x_table, NT)
    value = jnp.zeros((1, NX), F32)
    for z in range(NZ):
        value = factor_b[pl.ds(z, 1)] - factor_a[pl.ds(z, 1)] * value
        factor_b[pl.ds(z, 1)] = value
    value = jnp.zeros((1, NX), F32)
    for z in reversed(range(NZ)):
        value = factor_b[pl.ds(z, 1)] - factor_c[pl.ds(z, 1)] * value
        factor_b[pl.ds(z, 1)] = value
    solved = times_table(factor_b[...], x_table, NN)
    for slot, lined in ((0, solved), (1, z_slope(solved, metric_rows))):
        for part in range(4):
            spread[slot, part] = lined[:, part * LANES : part * LANES + LANES]

        def send_back(px, pz):
            remote(
                spread.at[slot, px, pl.ds(pz, 1)],
                returned.at[slot, pl.ds(me, 1)],
                back_send.at[slot],
                back_recv.at[slot],
                px * 64 + pz,
            ).start()

        each_peer(send_back)
        returned[slot, pl.ds(me, 1)] = spread[slot, group, pl.ds(layer, 1)]

    finish(back_recv.at[0])
    rows = returned[0]
    edges[2, :, :NY] = edge_lines(rows)
    p_edges = send_edges(2, NY)
    field = table_times(y_inverse, rows)
    pressure[0] = field
    after, before = y_neighbours(field)
    new_velocity[1, 0] = partial[1] - (0.5 * TIME_STEP) * (after - before)
    for copy in p_edges:
        copy.wait()
    after, before = lined_x(rows, edge_pair(2, 0))
    new_velocity[0, 0] = partial[0] - TIME_STEP * table_times(y_inverse, 0.5 * (after - before))
    finish(back_recv.at[1])
    new_velocity[2, 0] = partial[2] - TIME_STEP * table_times(y_inverse, returned[1])
    for slot in range(2):
        finish(out_send.at[slot])
        finish(back_send.at[slot])


def publish_kernel(step_in, pressure_in, step_out, pressure_out, sems):
    copies = (
        pltpu.make_async_copy(step_in, step_out, sems.at[0]),
        pltpu.make_async_copy(pressure_in, pressure_out, sems.at[1]),
    )
    for copy in copies:
        copy.start()
    for copy in copies:
        copy.wait()


def per_device(velocity, earlier_term, face_metric):
    y_cosines = cosine_table(NY)
    y_squares = (np.arange(NY) * (math.pi / NY)) ** 2
    y_second = -(y_cosines.T * y_squares) @ y_cosines
    vmem = pl.BlockSpec(memory_space=pltpu.VMEM)
    hbm = pl.BlockSpec(memory_space=pltpu.HBM)
    dma = pltpu.SemaphoreType.DMA
    arrays = [
        pltpu.with_memory_space_constraint(array, pltpu.HBM)
        for array in (
            velocity,
            earlier_term,
            jnp.asarray(halves(y_second)),
            jnp.asarray(halves(y_cosines)),
            jnp.asarray(halves(y_cosines.T)),
            jnp.asarray(halves(cosine_table(NX))),
        )
    ]
    stepped = pl.pallas_call(
        step_kernel,
        out_shape=(
            jax.ShapeDtypeStruct(velocity.shape, F32),
            jax.ShapeDtypeStruct(velocity.shape[1:], F32),
        ),
        in_specs=[pl.BlockSpec(memory_space=pltpu.SMEM)] + [hbm] * 6,
        out_specs=(vmem, vmem),
        scratch_shapes=[
            pltpu.VMEM((3, 1, NY, LANES), F32),
            pltpu.VMEM((3, 1, NY, LANES), BF16),
            pltpu.VMEM((2, NY, NY), BF16),
            pltpu.VMEM((2, NY, NY), BF16),
            pltpu.VMEM((2, NY, NY), BF16),
            pltpu.VMEM((2, NX, NX), BF16),
            pltpu.VMEM((3, 8, 3 * NY), F32),
            pltpu.VMEM((3, 2, 8, 3 * NY), F32),
            pltpu.VMEM((2, 8, 3 * NY), F32),
            pltpu.VMEM((3, NY, LANES), F32),
            pltpu.VMEM((3, NY, LANES), F32),
            pltpu.VMEM((3, NY, LANES), F32),
            pltpu.VMEM((2, NY, LANES), F32),
            pltpu.VMEM((2, 4, NZ, LANES), F32),
            pltpu.VMEM((NZ, LANES), F32),
            pltpu.VMEM((NZ, NX), F32),
            pltpu.VMEM((NZ, NX), F32),
            pltpu.VMEM((NZ, NX), F32),
            pltpu.VMEM((2, 4, NZ, LANES), F32),
            pltpu.VMEM((2, NY, LANES), F32),
            dma((8,)),
            dma((4, 2)),
            dma((4, 2)),
            dma((2, 3)),
            dma((2, 3)),
            dma((2,)),
            dma((2,)),
            dma((2,)),
            dma((2,)),
            pltpu.SemaphoreType.REGULAR,
            pltpu.SemaphoreType.REGULAR,
        ],
        compiler_params=pltpu.CompilerParams(
            collective_id=0, has_side_effects=True, vmem_limit_bytes=16 << 20
        ),
    )(pltpu.with_memory_space_constraint(face_metric, pltpu.HBM), *arrays)
    return pl.pallas_call(
        publish_kernel,
        out_shape=tuple(jax.ShapeDtypeStruct(a.shape, a.dtype) for a in stepped),
        in_specs=[vmem, vmem],
        out_specs=(hbm, hbm),
        scratch_shapes=[dma((2,))],
        compiler_params=pltpu.CompilerParams(vmem_limit_bytes=4 << 20),
    )(*stepped)


def solution(mesh):
    placed = (P(None, "gz", None, "gx"), P(None, "gz", None, "gx"), P())
    return jax.shard_map(
        per_device,
        mesh=mesh,
        in_specs=placed,
        out_specs=(P(None, "gz", None, "gx"), P("gz", None, "gx")),
        check_vma=False,
    )
```

```python
import math

import jax
import jax.numpy as jnp
import numpy as np
from jax import lax
from jax.experimental import pallas as pl
from jax.experimental.pallas import tpu as pltpu
from jax.sharding import PartitionSpec as P

TIME_STEP = 0.4
ADVECT_WEIGHT = 5.0 / 12.0
EARLIER_WEIGHT = -17.0 / 60.0
VISCOUS_WEIGHT = 2.0 / 15.0
NX = 512
NY = 256
NZ = 64
LANES = 128
PEERS = 256
LOGICAL = pl.DeviceIdType.LOGICAL
F32 = jnp.float32
BF16 = jnp.bfloat16
NN = (((1,), (0,)), ((), ()))
NT = (((1,), (1,)), ((), ()))
TN = (((0,), (0,)), ((), ()))


def hops(shift):
    return min(shift[0], 4 - shift[0]) + min(shift[1], 4 - shift[1]) + min(shift[2], 8 - shift[2])


SHIFTS = sorted(
    (
        (i, k, j, m)
        for m in (1, 0)
        for j in (4, 3, 5, 2, 6, 1, 7, 0)
        for k in (2, 1, 3, 0)
        for i in (2, 1, 3, 0)
        if (i, k, j, m) != (0, 0, 0, 0)
    ),
    key=lambda shift: -hops(shift),
)


def cosine_table(extent):
    wavenumber = np.arange(extent)[:, None]
    points = np.arange(extent)[None, :]
    residue = wavenumber * (2 * points + 1) % (4 * extent)
    cosines = np.cos(residue * (math.pi / (2 * extent))) * math.sqrt(2.0 / extent)
    cosines[0] *= math.sqrt(0.5)
    return cosines


def halves(table):
    high = table.astype(np.float32).astype(jnp.bfloat16)
    low = (table - high.astype(np.float64)).astype(np.float32).astype(jnp.bfloat16)
    return np.stack([high, low])


def split(values):
    high = values.astype(BF16)
    low = (values - high.astype(F32)).astype(BF16)
    return high, low


def mul(a, b, dims):
    return lax.dot_general(a, b, dims, preferred_element_type=F32)


def table_times(table, values):
    high, low = split(values)
    t_high, t_low = table[0], table[1]
    return mul(t_high, high, NN) + (mul(t_high, low, NN) + mul(t_low, high, NN))


def times_table(values, table, dims):
    high, low = split(values)
    t_high, t_low = table[0], table[1]
    return mul(high, t_high, dims) + (mul(high, t_low, dims) + mul(low, t_high, dims))


def row_ids(shape):
    return lax.broadcasted_iota(jnp.int32, shape, 0)


def lane_ids(shape):
    return lax.broadcasted_iota(jnp.int32, shape, 1)


def y_neighbours(field):
    rows = row_ids(field.shape)
    count = field.shape[0]
    after = jnp.where(rows == count - 1, field, pltpu.roll(field, count - 1, 0))
    before = jnp.where(rows == 0, field, pltpu.roll(field, 1, 0))
    return after, before


def z_slope(columns, metric):
    rows = row_ids(columns.shape)
    count = columns.shape[0]
    after = jnp.where(rows == count - 1, 0.0, pltpu.roll(columns, count - 1, 0))
    before = jnp.where(rows == 0, 0.0, pltpu.roll(columns, 1, 0))
    return metric * (0.5 * (after - before))


def x_slope(lines):
    count = lines.shape[1]
    return 0.5 * (pltpu.roll(lines, count - 1, 1) - pltpu.roll(lines, 1, 1))


def lined_x(field, edge_rows):
    shape = (16, LANES)
    places = (row_ids(shape) == 1) & (lane_ids(shape) == 0)
    places |= (row_ids(shape) == 8) & (lane_ids(shape) == LANES - 1)
    places = places.astype(F32).astype(BF16)
    high, low = split(edge_rows)
    outer = mul(high, places, TN) + mul(low, places, TN)
    lanes = lane_ids(field.shape)
    after = jnp.where(lanes == LANES - 1, outer, pltpu.roll(field, LANES - 1, 1))
    before = jnp.where(lanes == 0, outer, pltpu.roll(field, 1, 1))
    return after, before


def edge_lines(field):
    shape = (8, LANES)
    picks = (row_ids(shape) == 0) & (lane_ids(shape) == 0)
    picks |= (row_ids(shape) == 1) & (lane_ids(shape) == LANES - 1)
    picks = picks.astype(F32).astype(BF16)
    high, low = split(field)
    return mul(picks, high, NT) + mul(picks, low, NT)


def step_kernel(
    faces,
    velocity_in,
    earlier_in,
    y_second_in,
    y_forward_in,
    y_inverse_in,
    x_table_in,
    new_velocity,
    pressure,
    velocity,
    earlier,
    y_second,
    y_forward,
    y_inverse,
    x_table,
    edges,
    edges_in,
    edges_z,
    below,
    above,
    partial,
    y_rows,
    gathered,
    metrics,
    factor_c,
    factor_a,
    factor_b,
    spread,
    returned,
    load_sem,
    edge_send,
    edge_recv,
    halo_send,
    halo_recv,
    out_send,
    out_recv,
    back_send,
    back_recv,
    plane_token,
    line_token,
):
    loads = [
        pltpu.make_async_copy(source, target, load_sem.at[i])
        for i, (source, target) in enumerate(
            (
                (velocity_in.at[0], velocity.at[0]),
                (velocity_in.at[2], velocity.at[2]),
                (velocity_in.at[1], velocity.at[1]),
                (y_second_in, y_second),
                (earlier_in, earlier),
                (y_forward_in, y_forward),
                (x_table_in, x_table),
                (y_inverse_in, y_inverse),
            )
        )
    ]
    for load in loads[:3]:
        load.start()

    group = lax.axis_index("gx")
    layer = lax.axis_index("gz")
    me = group * 64 + layer
    y_parts = [((layer & 6) + (shift << 1)) & 6 for shift in range(4)]
    core_parts = [layer & 1, (layer & 1) ^ 1]
    x_parts = [(group + shift) & 3 for shift in range(4)]
    x_line = [x_parts[i] * 64 + layer for i in (1, 3, 2)]
    y_line = [
        group * 64 + ((layer & 56) | (y_parts[k] | core_parts[m]))
        for k, m in ((0, 1), (1, 0), (1, 1), (3, 0), (3, 1), (2, 0), (2, 1))
    ]
    z_line = [
        group * 64 + (((layer & 56) + (shift << 3)) & 56) + (layer & 7)
        for shift in (1, 7, 2, 6, 3, 5, 4)
    ]
    x_right, x_left = x_line[0], x_line[1]
    z_up = group * 64 + ((layer + 1) & 63)
    z_down = group * 64 + ((layer + 63) & 63)
    at_top = (layer & 7) == 7
    at_bottom = (layer & 7) == 0

    def tell(sem, peer):
        pl.semaphore_signal(sem, inc=1, device_id=peer, device_id_type=LOGICAL)

    z_parts = [((layer & 56) + (shift << 3)) & 56 for shift in range(8)]

    def each_peer(act):
        for i, k, j, m in SHIFTS:
            act(x_parts[i], z_parts[j] | (y_parts[k] | core_parts[m]))

    def remote(source, target, send, recv, peer):
        return pltpu.make_async_remote_copy(
            src_ref=source,
            dst_ref=target,
            send_sem=send,
            recv_sem=recv,
            device_id=peer,
            device_id_type=LOGICAL,
        )

    barrier = pltpu.get_barrier_semaphore()

    @pl.when(at_top)
    def _():
        tell(barrier, z_up)

    @pl.when(at_bottom)
    def _():
        tell(barrier, z_down)

    for peer in y_line + x_line + z_line:
        tell(barrier, peer)
    for i in range(3):
        loads[i].wait()
    for load in loads[3:]:
        load.start()
    for c in range(3):
        edges[0, :, c * NY : c * NY + NY] = edge_lines(velocity[c, 0])
    pl.semaphore_wait(
        barrier, 17 + jnp.where(at_top, 1, 0) + jnp.where(at_bottom, 1, 0)
    )

    def send_edges(k, width):
        copies = []
        for side, peer in enumerate((x_right, x_left)):
            copies.append(
                remote(
                    edges.at[k, :, pl.ds(0, width)],
                    edges_in.at[k, side, :, pl.ds(0, width)],
                    edge_send.at[k, side],
                    edge_recv.at[k, side],
                    peer,
                )
            )
            copies[-1].start()
        return copies

    def edge_pair(k, first):
        part = slice(first, first + NY)
        return jnp.concatenate([edges_in[k, 0, :, part], edges_in[k, 1, :, part]], 0)

    velocity_edges = send_edges(0, 3 * NY)
    layer_edges = []
    for side, peer in enumerate((z_up, z_down)):
        layer_edges.append(
            remote(
                edges.at[0], edges_z.at[side], edge_send.at[3, side], edge_recv.at[3, side], peer
            )
        )
        layer_edges[-1].start()
    halos = {}
    for c in (2, 0, 1):
        up = remote(velocity.at[c, 0], below.at[c], halo_send.at[0, c], halo_recv.at[0, c], z_up)
        down = remote(velocity.at[c, 0], above.at[c], halo_send.at[1, c], halo_recv.at[1, c], z_down)
        up.start()
        down.start()
        halos[c] = (up, down)
    for peer in y_line:
        tell(plane_token, peer)

    u = velocity[0, 0]
    v = velocity[1, 0]
    loads[3].wait()
    loads[4].wait()
    for c in (0, 2, 1):
        field = velocity[c, 0]
        after, before = y_neighbours(field)
        bend = table_times(y_second, field) - 2.0 * field
        partial[c] = field + TIME_STEP * (
            EARLIER_WEIGHT * earlier[c, 0].astype(F32)
            + VISCOUS_WEIGHT * bend
            - ADVECT_WEIGHT * (v * (0.5 * (after - before)))
        )

    pl.semaphore_wait(plane_token, 7)
    for peer in x_line:
        tell(line_token, peer)

    lower = faces[0, layer]
    upper = faces[1, layer]
    metric = 0.5 * (lower + upper)
    w = velocity[2, 0]

    def with_z(base, field, below_it, above_it, drift):
        after = jnp.where(layer == NZ - 1, 0.0, above_it)
        before = jnp.where(layer == 0, 0.0, below_it)
        bend = metric * (upper * (after - field) - lower * (field - before))
        return base + TIME_STEP * (
            VISCOUS_WEIGHT * bend - ADVECT_WEIGHT * (drift * (metric * (0.5 * (after - before))))
        )

    def add_x(c):
        after, before = lined_x(velocity[c, 0], edge_pair(0, c * NY))
        partial[c] = partial[c] + TIME_STEP * (
            VISCOUS_WEIGHT * (after + before) - ADVECT_WEIGHT * (u * (0.5 * (after - before)))
        )

    def predict(c):
        for copy in halos[c]:
            copy.wait()
        predicted = with_z(partial[c], velocity[c, 0], below[c], above[c], w)
        partial[c] = predicted
        return predicted

    for copy in velocity_edges:
        copy.wait()
    add_x(0)
    own = edge_lines(partial[0])
    for copy in layer_edges:
        copy.wait()
    edges[1, :, :NY] = with_z(
        own,
        edges[0, :, :NY],
        edges_z[0, :, :NY],
        edges_z[1, :, :NY],
        edges[0, :, 2 * NY :],
    )
    u_edges = send_edges(1, NY)
    add_x(2)
    add_x(1)
    loads[5].wait()

    def send_rows(slot, field):
        y_rows[slot] = table_times(y_forward, field)

        def send(px, pz):
            peer = px * 64 + pz
            remote(
                y_rows.at[slot, pl.ds(peer, 1)],
                gathered.at[slot, group, pl.ds(layer, 1)],
                out_send.at[slot],
                out_recv.at[slot],
                peer,
            ).start()

        each_peer(send)
        gathered[slot, group, pl.ds(layer, 1)] = y_rows[slot, pl.ds(me, 1)]

    predicted_w = predict(2)
    pl.semaphore_wait(line_token, 3)
    send_rows(0, predicted_w)
    predicted_u = predict(0)
    for copy in u_edges:
        copy.wait()
    after, before = lined_x(predicted_u, edge_pair(1, 0))
    flow = after - before
    after, before = y_neighbours(predict(1))
    send_rows(1, 0.5 * (flow + (after - before)))

    k_y = me.astype(F32) * (math.pi / NY)
    k_x = lane_ids((1, NX)).astype(F32) * (math.pi / NX)
    eigen = k_y * k_y + k_x * k_x
    ratio = jnp.zeros((1, NX), F32)
    for z in range(NZ):
        lower = faces[0, z]
        upper = faces[1, z]
        metrics[pl.ds(z, 1)] = jnp.full((1, LANES), 0.5 * (lower + upper), F32)
        per_metric = 2.0 / jnp.full((1, NX), lower + upper, F32)
        inverse = 1.0 / (-(lower + upper) - eigen * per_metric - lower * ratio)
        ratio = upper * inverse
        factor_c[pl.ds(z, 1)] = ratio
        factor_a[pl.ds(z, 1)] = lower * inverse
        factor_b[pl.ds(z, 1)] = (per_metric * inverse) * (1.0 / TIME_STEP)
    metric_rows = jnp.concatenate([metrics[...]] * 4, 1)
    loads[6].wait()
    loads[7].wait()

    others = returned.at[0, pl.ds(0, PEERS - 1)]

    def finish(sem):
        pltpu.make_async_copy(others, others, sem).wait()

    def lines(slot):
        return jnp.concatenate([gathered[slot, part] for part in range(4)], 1)

    finish(out_recv.at[0])
    source = z_slope(lines(0), metric_rows)
    finish(out_recv.at[1])
    source = source + lines(1)
    factor_b[...] = factor_b[...] * times_table(source, x_table, NT)
    value = jnp.zeros((1, NX), F32)
    for z in range(NZ):
        value = factor_b[pl.ds(z, 1)] - factor_a[pl.ds(z, 1)] * value
        factor_b[pl.ds(z, 1)] = value
    value = jnp.zeros((1, NX), F32)
    for z in reversed(range(NZ)):
        value = factor_b[pl.ds(z, 1)] - factor_c[pl.ds(z, 1)] * value
        factor_b[pl.ds(z, 1)] = value
    solved = times_table(factor_b[...], x_table, NN)
    for slot, lined in ((0, solved), (1, z_slope(solved, metric_rows))):
        for part in range(4):
            spread[slot, part] = lined[:, part * LANES : part * LANES + LANES]

        def send_back(px, pz):
            remote(
                spread.at[slot, px, pl.ds(pz, 1)],
                returned.at[slot, pl.ds(me, 1)],
                back_send.at[slot],
                back_recv.at[slot],
                px * 64 + pz,
            ).start()

        each_peer(send_back)
        returned[slot, pl.ds(me, 1)] = spread[slot, group, pl.ds(layer, 1)]

    finish(back_recv.at[0])
    rows = returned[0]
    edges[2, :, :NY] = edge_lines(rows)
    p_edges = send_edges(2, NY)
    field = table_times(y_inverse, rows)
    pressure[0] = field
    after, before = y_neighbours(field)
    new_velocity[1, 0] = partial[1] - (0.5 * TIME_STEP) * (after - before)
    finish(back_recv.at[1])
    new_velocity[2, 0] = partial[2] - TIME_STEP * table_times(y_inverse, returned[1])
    for copy in p_edges:
        copy.wait()
    after, before = lined_x(rows, edge_pair(2, 0))
    new_velocity[0, 0] = partial[0] - TIME_STEP * table_times(y_inverse, 0.5 * (after - before))
    for slot in range(2):
        finish(out_send.at[slot])
        finish(back_send.at[slot])


def publish_kernel(step_in, pressure_in, step_out, pressure_out, sems):
    copies = (
        pltpu.make_async_copy(step_in, step_out, sems.at[0]),
        pltpu.make_async_copy(pressure_in, pressure_out, sems.at[1]),
    )
    for copy in copies:
        copy.start()
    for copy in copies:
        copy.wait()


def per_device(velocity, earlier_term, face_metric):
    y_cosines = cosine_table(NY)
    y_squares = (np.arange(NY) * (math.pi / NY)) ** 2
    y_second = -(y_cosines.T * y_squares) @ y_cosines
    vmem = pl.BlockSpec(memory_space=pltpu.VMEM)
    hbm = pl.BlockSpec(memory_space=pltpu.HBM)
    dma = pltpu.SemaphoreType.DMA
    arrays = [
        pltpu.with_memory_space_constraint(array, pltpu.HBM)
        for array in (
            velocity,
            earlier_term,
            jnp.asarray(halves(y_second)),
            jnp.asarray(halves(y_cosines)),
            jnp.asarray(halves(y_cosines.T)),
            jnp.asarray(halves(cosine_table(NX))),
        )
    ]
    stepped = pl.pallas_call(
        step_kernel,
        out_shape=(
            jax.ShapeDtypeStruct(velocity.shape, F32),
            jax.ShapeDtypeStruct(velocity.shape[1:], F32),
        ),
        in_specs=[pl.BlockSpec(memory_space=pltpu.SMEM)] + [hbm] * 6,
        out_specs=(vmem, vmem),
        scratch_shapes=[
            pltpu.VMEM((3, 1, NY, LANES), F32),
            pltpu.VMEM((3, 1, NY, LANES), BF16),
            pltpu.VMEM((2, NY, NY), BF16),
            pltpu.VMEM((2, NY, NY), BF16),
            pltpu.VMEM((2, NY, NY), BF16),
            pltpu.VMEM((2, NX, NX), BF16),
            pltpu.VMEM((3, 8, 3 * NY), F32),
            pltpu.VMEM((3, 2, 8, 3 * NY), F32),
            pltpu.VMEM((2, 8, 3 * NY), F32),
            pltpu.VMEM((3, NY, LANES), F32),
            pltpu.VMEM((3, NY, LANES), F32),
            pltpu.VMEM((3, NY, LANES), F32),
            pltpu.VMEM((2, NY, LANES), F32),
            pltpu.VMEM((2, 4, NZ, LANES), F32),
            pltpu.VMEM((NZ, LANES), F32),
            pltpu.VMEM((NZ, NX), F32),
            pltpu.VMEM((NZ, NX), F32),
            pltpu.VMEM((NZ, NX), F32),
            pltpu.VMEM((2, 4, NZ, LANES), F32),
            pltpu.VMEM((2, NY, LANES), F32),
            dma((8,)),
            dma((4, 2)),
            dma((4, 2)),
            dma((2, 3)),
            dma((2, 3)),
            dma((2,)),
            dma((2,)),
            dma((2,)),
            dma((2,)),
            pltpu.SemaphoreType.REGULAR,
            pltpu.SemaphoreType.REGULAR,
        ],
        compiler_params=pltpu.CompilerParams(
            collective_id=0, has_side_effects=True, vmem_limit_bytes=16 << 20
        ),
    )(pltpu.with_memory_space_constraint(face_metric, pltpu.HBM), *arrays)
    return pl.pallas_call(
        publish_kernel,
        out_shape=tuple(jax.ShapeDtypeStruct(a.shape, a.dtype) for a in stepped),
        in_specs=[vmem, vmem],
        out_specs=(hbm, hbm),
        scratch_shapes=[dma((2,))],
        compiler_params=pltpu.CompilerParams(vmem_limit_bytes=4 << 20),
    )(*stepped)


def solution(mesh):
    placed = (P(None, "gz", None, "gx"), P(None, "gz", None, "gx"), P())
    return jax.shard_map(
        per_device,
        mesh=mesh,
        in_specs=placed,
        out_specs=(P(None, "gz", None, "gx"), P("gz", None, "gx")),
        check_vma=False,
    )
```

```python
import math

import jax
import jax.numpy as jnp
import numpy as np
from jax import lax
from jax.experimental import pallas as pl
from jax.experimental.pallas import tpu as pltpu
from jax.sharding import PartitionSpec as P

TIME_STEP = 0.4
ADVECT_WEIGHT = 5.0 / 12.0
EARLIER_WEIGHT = -17.0 / 60.0
VISCOUS_WEIGHT = 2.0 / 15.0
NX = 512
NY = 256
NZ = 64
LANES = 128
PEERS = 256
LOGICAL = pl.DeviceIdType.LOGICAL
F32 = jnp.float32
BF16 = jnp.bfloat16
NN = (((1,), (0,)), ((), ()))
NT = (((1,), (1,)), ((), ()))
TN = (((0,), (0,)), ((), ()))


def hops(shift):
    return min(shift[0], 4 - shift[0]) + min(shift[1], 4 - shift[1]) + min(shift[2], 8 - shift[2])


SHIFTS = sorted(
    (
        (i, k, j, m)
        for m in (1, 0)
        for j in (4, 3, 5, 2, 6, 1, 7, 0)
        for k in (2, 1, 3, 0)
        for i in (2, 1, 3, 0)
        if (i, k, j, m) != (0, 0, 0, 0)
    ),
    key=lambda shift: -hops(shift),
)


def cosine_table(extent):
    wavenumber = np.arange(extent)[:, None]
    points = np.arange(extent)[None, :]
    residue = wavenumber * (2 * points + 1) % (4 * extent)
    cosines = np.cos(residue * (math.pi / (2 * extent))) * math.sqrt(2.0 / extent)
    cosines[0] *= math.sqrt(0.5)
    return cosines


def halves(table):
    high = table.astype(np.float32).astype(jnp.bfloat16)
    low = (table - high.astype(np.float64)).astype(np.float32).astype(jnp.bfloat16)
    return np.stack([high, low])


def split(values):
    high = values.astype(BF16)
    low = (values - high.astype(F32)).astype(BF16)
    return high, low


def mul(a, b, dims):
    return lax.dot_general(a, b, dims, preferred_element_type=F32)


def table_times(table, values):
    high, low = split(values)
    t_high, t_low = table[0], table[1]
    return mul(t_high, high, NN) + (mul(t_high, low, NN) + mul(t_low, high, NN))


def times_table(values, table, dims):
    high, low = split(values)
    t_high, t_low = table[0], table[1]
    return mul(high, t_high, dims) + (mul(high, t_low, dims) + mul(low, t_high, dims))


def row_ids(shape):
    return lax.broadcasted_iota(jnp.int32, shape, 0)


def lane_ids(shape):
    return lax.broadcasted_iota(jnp.int32, shape, 1)


def y_neighbours(field):
    rows = row_ids(field.shape)
    count = field.shape[0]
    after = jnp.where(rows == count - 1, field, pltpu.roll(field, count - 1, 0))
    before = jnp.where(rows == 0, field, pltpu.roll(field, 1, 0))
    return after, before


def z_slope(columns, metric):
    rows = row_ids(columns.shape)
    count = columns.shape[0]
    after = jnp.where(rows == count - 1, 0.0, pltpu.roll(columns, count - 1, 0))
    before = jnp.where(rows == 0, 0.0, pltpu.roll(columns, 1, 0))
    return metric * (0.5 * (after - before))


def x_slope(lines):
    count = lines.shape[1]
    return 0.5 * (pltpu.roll(lines, count - 1, 1) - pltpu.roll(lines, 1, 1))


def lined_x(field, edge_rows):
    shape = (16, LANES)
    places = (row_ids(shape) == 1) & (lane_ids(shape) == 0)
    places |= (row_ids(shape) == 8) & (lane_ids(shape) == LANES - 1)
    places = places.astype(F32).astype(BF16)
    high, low = split(edge_rows)
    outer = mul(high, places, TN) + mul(low, places, TN)
    lanes = lane_ids(field.shape)
    after = jnp.where(lanes == LANES - 1, outer, pltpu.roll(field, LANES - 1, 1))
    before = jnp.where(lanes == 0, outer, pltpu.roll(field, 1, 1))
    return after, before


def edge_lines(field):
    shape = (8, LANES)
    picks = (row_ids(shape) == 0) & (lane_ids(shape) == 0)
    picks |= (row_ids(shape) == 1) & (lane_ids(shape) == LANES - 1)
    picks = picks.astype(F32).astype(BF16)
    high, low = split(field)
    return mul(picks, high, NT) + mul(picks, low, NT)


def step_kernel(
    faces,
    velocity_in,
    earlier_in,
    y_second_in,
    y_forward_in,
    y_inverse_in,
    x_table_in,
    new_velocity,
    pressure,
    velocity,
    earlier,
    y_second,
    y_forward,
    y_inverse,
    x_table,
    edges,
    edges_in,
    edges_z,
    below,
    above,
    partial,
    y_rows,
    gathered,
    metrics,
    factor_c,
    factor_a,
    factor_b,
    middle,
    spread,
    returned,
    load_sem,
    edge_send,
    edge_recv,
    halo_send,
    halo_recv,
    out_send,
    out_recv,
    back_send,
    back_recv,
    plane_token,
    line_token,
):
    loads = [
        pltpu.make_async_copy(source, target, load_sem.at[i])
        for i, (source, target) in enumerate(
            (
                (velocity_in.at[0], velocity.at[0]),
                (velocity_in.at[2], velocity.at[2]),
                (velocity_in.at[1], velocity.at[1]),
                (y_second_in, y_second),
                (earlier_in, earlier),
                (y_forward_in, y_forward),
                (x_table_in, x_table),
                (y_inverse_in, y_inverse),
            )
        )
    ]
    for load in loads[:3]:
        load.start()

    group = lax.axis_index("gx")
    layer = lax.axis_index("gz")
    me = group * 64 + layer
    y_parts = [((layer & 6) + (shift << 1)) & 6 for shift in range(4)]
    core_parts = [layer & 1, (layer & 1) ^ 1]
    x_parts = [(group + shift) & 3 for shift in range(4)]
    x_line = [x_parts[i] * 64 + layer for i in (1, 3, 2)]
    y_line = [
        group * 64 + ((layer & 56) | (y_parts[k] | core_parts[m]))
        for k, m in ((0, 1), (1, 0), (1, 1), (3, 0), (3, 1), (2, 0), (2, 1))
    ]
    z_line = [
        group * 64 + (((layer & 56) + (shift << 3)) & 56) + (layer & 7)
        for shift in (1, 7, 2, 6, 3, 5, 4)
    ]
    x_right, x_left = x_line[0], x_line[1]
    z_up = group * 64 + ((layer + 1) & 63)
    z_down = group * 64 + ((layer + 63) & 63)
    at_top = (layer & 7) == 7
    at_bottom = (layer & 7) == 0

    def tell(sem, peer):
        pl.semaphore_signal(sem, inc=1, device_id=peer, device_id_type=LOGICAL)

    z_parts = [((layer & 56) + (shift << 3)) & 56 for shift in range(8)]

    def each_peer(act):
        for i, k, j, m in SHIFTS:
            act(x_parts[i], z_parts[j] | (y_parts[k] | core_parts[m]))

    def remote(source, target, send, recv, peer):
        return pltpu.make_async_remote_copy(
            src_ref=source,
            dst_ref=target,
            send_sem=send,
            recv_sem=recv,
            device_id=peer,
            device_id_type=LOGICAL,
        )

    barrier = pltpu.get_barrier_semaphore()

    @pl.when(at_top)
    def _():
        tell(barrier, z_up)

    @pl.when(at_bottom)
    def _():
        tell(barrier, z_down)

    for peer in y_line + x_line + z_line:
        tell(barrier, peer)
    for i in range(3):
        loads[i].wait()
    for load in loads[3:]:
        load.start()
    for c in range(3):
        edges[0, :, c * NY : c * NY + NY] = edge_lines(velocity[c, 0])
    pl.semaphore_wait(
        barrier, 17 + jnp.where(at_top, 1, 0) + jnp.where(at_bottom, 1, 0)
    )

    def send_edges(k, width):
        copies = []
        for side, peer in enumerate((x_right, x_left)):
            copies.append(
                remote(
                    edges.at[k, :, pl.ds(0, width)],
                    edges_in.at[k, side, :, pl.ds(0, width)],
                    edge_send.at[k, side],
                    edge_recv.at[k, side],
                    peer,
                )
            )
            copies[-1].start()
        return copies

    def edge_pair(k, first):
        part = slice(first, first + NY)
        return jnp.concatenate([edges_in[k, 0, :, part], edges_in[k, 1, :, part]], 0)

    velocity_edges = send_edges(0, 3 * NY)
    layer_edges = []
    for side, peer in enumerate((z_up, z_down)):
        layer_edges.append(
            remote(
                edges.at[0], edges_z.at[side], edge_send.at[3, side], edge_recv.at[3, side], peer
            )
        )
        layer_edges[-1].start()
    halos = {}
    for c in (2, 0, 1):
        up = remote(velocity.at[c, 0], below.at[c], halo_send.at[0, c], halo_recv.at[0, c], z_up)
        down = remote(velocity.at[c, 0], above.at[c], halo_send.at[1, c], halo_recv.at[1, c], z_down)
        up.start()
        down.start()
        halos[c] = (up, down)
    for peer in y_line:
        tell(plane_token, peer)

    u = velocity[0, 0]
    v = velocity[1, 0]
    loads[3].wait()
    loads[4].wait()
    for c in (0, 2, 1):
        field = velocity[c, 0]
        after, before = y_neighbours(field)
        bend = table_times(y_second, field) - 2.0 * field
        partial[c] = field + TIME_STEP * (
            EARLIER_WEIGHT * earlier[c, 0].astype(F32)
            + VISCOUS_WEIGHT * bend
            - ADVECT_WEIGHT * (v * (0.5 * (after - before)))
        )

    pl.semaphore_wait(plane_token, 7)
    for peer in x_line:
        tell(line_token, peer)

    lower = faces[0, layer]
    upper = faces[1, layer]
    metric = 0.5 * (lower + upper)
    w = velocity[2, 0]

    def with_z(base, field, below_it, above_it, drift):
        after = jnp.where(layer == NZ - 1, 0.0, above_it)
        before = jnp.where(layer == 0, 0.0, below_it)
        bend = metric * (upper * (after - field) - lower * (field - before))
        return base + TIME_STEP * (
            VISCOUS_WEIGHT * bend - ADVECT_WEIGHT * (drift * (metric * (0.5 * (after - before))))
        )

    def add_x(c):
        after, before = lined_x(velocity[c, 0], edge_pair(0, c * NY))
        partial[c] = partial[c] + TIME_STEP * (
            VISCOUS_WEIGHT * (after + before) - ADVECT_WEIGHT * (u * (0.5 * (after - before)))
        )

    def predict(c):
        for copy in halos[c]:
            copy.wait()
        predicted = with_z(partial[c], velocity[c, 0], below[c], above[c], w)
        partial[c] = predicted
        return predicted

    for copy in velocity_edges:
        copy.wait()
    add_x(0)
    own = edge_lines(partial[0])
    for copy in layer_edges:
        copy.wait()
    edges[1, :, :NY] = with_z(
        own,
        edges[0, :, :NY],
        edges_z[0, :, :NY],
        edges_z[1, :, :NY],
        edges[0, :, 2 * NY :],
    )
    u_edges = send_edges(1, NY)
    add_x(2)
    add_x(1)
    loads[5].wait()

    def send_rows(slot, field):
        y_rows[slot] = table_times(y_forward, field)

        def send(px, pz):
            peer = px * 64 + pz
            remote(
                y_rows.at[slot, pl.ds(peer, 1)],
                gathered.at[slot, group, pl.ds(layer, 1)],
                out_send.at[slot],
                out_recv.at[slot],
                peer,
            ).start()

        each_peer(send)
        gathered[slot, group, pl.ds(layer, 1)] = y_rows[slot, pl.ds(me, 1)]

    predicted_w = predict(2)
    pl.semaphore_wait(line_token, 3)
    send_rows(0, predicted_w)
    predicted_u = predict(0)
    for copy in u_edges:
        copy.wait()
    after, before = lined_x(predicted_u, edge_pair(1, 0))
    flow = after - before
    after, before = y_neighbours(predict(1))
    send_rows(1, 0.5 * (flow + (after - before)))

    k_y = me.astype(F32) * (math.pi / NY)
    k_x = lane_ids((1, NX)).astype(F32) * (math.pi / NX)
    eigen = k_y * k_y + k_x * k_x

    def factor_row(z, ratio, inner, outer):
        total = faces[0, z] + faces[1, z]
        metrics[pl.ds(z, 1)] = jnp.full((1, LANES), 0.5 * total, F32)
        per_metric = 2.0 / jnp.full((1, NX), total, F32)
        inverse = 1.0 / (-total - eigen * per_metric - inner * ratio)
        ratio = outer * inverse
        factor_c[pl.ds(z, 1)] = ratio
        factor_a[pl.ds(z, 1)] = inner * inverse
        factor_b[pl.ds(z, 1)] = (per_metric * inverse) * (1.0 / TIME_STEP)
        return ratio

    half = NZ // 2
    low_ratio = jnp.zeros((1, NX), F32)
    high_ratio = jnp.zeros((1, NX), F32)
    for z in range(half):
        low_ratio = factor_row(z, low_ratio, faces[0, z], faces[1, z])
        mirror = NZ - 1 - z
        high_ratio = factor_row(mirror, high_ratio, faces[1, mirror], faces[0, mirror])
    middle[...] = 1.0 / (1.0 - low_ratio * high_ratio)
    metric_rows = jnp.concatenate([metrics[...]] * 4, 1)
    loads[6].wait()
    loads[7].wait()

    others = returned.at[0, pl.ds(0, PEERS - 1)]

    def finish(sem):
        pltpu.make_async_copy(others, others, sem).wait()

    def lines(slot):
        return jnp.concatenate([gathered[slot, part] for part in range(4)], 1)

    finish(out_recv.at[0])
    source = z_slope(lines(0), metric_rows)
    finish(out_recv.at[1])
    source = source + lines(1)
    factor_b[...] = factor_b[...] * times_table(source, x_table, NT)
    low = jnp.zeros((1, NX), F32)
    high = jnp.zeros((1, NX), F32)
    for z in range(half):
        mirror = NZ - 1 - z
        low = factor_b[pl.ds(z, 1)] - factor_a[pl.ds(z, 1)] * low
        high = factor_b[pl.ds(mirror, 1)] - factor_a[pl.ds(mirror, 1)] * high
        factor_b[pl.ds(z, 1)] = low
        factor_b[pl.ds(mirror, 1)] = high
    low = (low - factor_c[pl.ds(half - 1, 1)] * high) * middle[...]
    high = high - factor_c[pl.ds(half, 1)] * low
    factor_b[pl.ds(half - 1, 1)] = low
    factor_b[pl.ds(half, 1)] = high
    for z in reversed(range(half - 1)):
        mirror = NZ - 1 - z
        low = factor_b[pl.ds(z, 1)] - factor_c[pl.ds(z, 1)] * low
        high = factor_b[pl.ds(mirror, 1)] - factor_c[pl.ds(mirror, 1)] * high
        factor_b[pl.ds(z, 1)] = low
        factor_b[pl.ds(mirror, 1)] = high
    solved = times_table(factor_b[...], x_table, NN)
    for slot, lined in ((0, solved), (1, z_slope(solved, metric_rows))):
        for part in range(4):
            spread[slot, part] = lined[:, part * LANES : part * LANES + LANES]

        def send_back(px, pz):
            remote(
                spread.at[slot, px, pl.ds(pz, 1)],
                returned.at[slot, pl.ds(me, 1)],
                back_send.at[slot],
                back_recv.at[slot],
                px * 64 + pz,
            ).start()

        each_peer(send_back)
        returned[slot, pl.ds(me, 1)] = spread[slot, group, pl.ds(layer, 1)]

    finish(back_recv.at[0])
    rows = returned[0]
    edges[2, :, :NY] = edge_lines(rows)
    p_edges = send_edges(2, NY)
    field = table_times(y_inverse, rows)
    pressure[0] = field
    lanes = lane_ids(rows.shape)
    after = jnp.where(lanes == LANES - 1, 0.0, pltpu.roll(rows, LANES - 1, 1))
    before = jnp.where(lanes == 0, 0.0, pltpu.roll(rows, 1, 1))
    inner_slope = table_times(y_inverse, 0.5 * (after - before))
    after, before = y_neighbours(field)
    new_velocity[1, 0] = partial[1] - (0.5 * TIME_STEP) * (after - before)
    finish(back_recv.at[1])
    new_velocity[2, 0] = partial[2] - TIME_STEP * table_times(y_inverse, returned[1])
    for copy in p_edges:
        copy.wait()
    shape = (16, LANES)
    places = jnp.where((row_ids(shape) == 8) & (lane_ids(shape) == LANES - 1), 0.5, 0.0)
    places = jnp.where((row_ids(shape) == 1) & (lane_ids(shape) == 0), -0.5, places).astype(BF16)
    high, low = split(times_table(edge_pair(2, 0), y_inverse, NT))
    slope = inner_slope + (mul(high, places, TN) + mul(low, places, TN))
    new_velocity[0, 0] = partial[0] - TIME_STEP * slope
    for slot in range(2):
        finish(out_send.at[slot])
        finish(back_send.at[slot])


def publish_kernel(step_in, pressure_in, step_out, pressure_out, sems):
    copies = (
        pltpu.make_async_copy(step_in, step_out, sems.at[0]),
        pltpu.make_async_copy(pressure_in, pressure_out, sems.at[1]),
    )
    for copy in copies:
        copy.start()
    for copy in copies:
        copy.wait()


def per_device(velocity, earlier_term, face_metric):
    y_cosines = cosine_table(NY)
    y_squares = (np.arange(NY) * (math.pi / NY)) ** 2
    y_second = -(y_cosines.T * y_squares) @ y_cosines
    vmem = pl.BlockSpec(memory_space=pltpu.VMEM)
    hbm = pl.BlockSpec(memory_space=pltpu.HBM)
    dma = pltpu.SemaphoreType.DMA
    arrays = [
        pltpu.with_memory_space_constraint(array, pltpu.HBM)
        for array in (
            velocity,
            earlier_term,
            jnp.asarray(halves(y_second)),
            jnp.asarray(halves(y_cosines)),
            jnp.asarray(halves(y_cosines.T)),
            jnp.asarray(halves(cosine_table(NX))),
        )
    ]
    stepped = pl.pallas_call(
        step_kernel,
        out_shape=(
            jax.ShapeDtypeStruct(velocity.shape, F32),
            jax.ShapeDtypeStruct(velocity.shape[1:], F32),
        ),
        in_specs=[pl.BlockSpec(memory_space=pltpu.SMEM)] + [hbm] * 6,
        out_specs=(vmem, vmem),
        scratch_shapes=[
            pltpu.VMEM((3, 1, NY, LANES), F32),
            pltpu.VMEM((3, 1, NY, LANES), BF16),
            pltpu.VMEM((2, NY, NY), BF16),
            pltpu.VMEM((2, NY, NY), BF16),
            pltpu.VMEM((2, NY, NY), BF16),
            pltpu.VMEM((2, NX, NX), BF16),
            pltpu.VMEM((3, 8, 3 * NY), F32),
            pltpu.VMEM((3, 2, 8, 3 * NY), F32),
            pltpu.VMEM((2, 8, 3 * NY), F32),
            pltpu.VMEM((3, NY, LANES), F32),
            pltpu.VMEM((3, NY, LANES), F32),
            pltpu.VMEM((3, NY, LANES), F32),
            pltpu.VMEM((2, NY, LANES), F32),
            pltpu.VMEM((2, 4, NZ, LANES), F32),
            pltpu.VMEM((NZ, LANES), F32),
            pltpu.VMEM((NZ, NX), F32),
            pltpu.VMEM((NZ, NX), F32),
            pltpu.VMEM((NZ, NX), F32),
            pltpu.VMEM((1, NX), F32),
            pltpu.VMEM((2, 4, NZ, LANES), F32),
            pltpu.VMEM((2, NY, LANES), F32),
            dma((8,)),
            dma((4, 2)),
            dma((4, 2)),
            dma((2, 3)),
            dma((2, 3)),
            dma((2,)),
            dma((2,)),
            dma((2,)),
            dma((2,)),
            pltpu.SemaphoreType.REGULAR,
            pltpu.SemaphoreType.REGULAR,
        ],
        compiler_params=pltpu.CompilerParams(
            collective_id=0, has_side_effects=True, vmem_limit_bytes=16 << 20
        ),
    )(pltpu.with_memory_space_constraint(face_metric, pltpu.HBM), *arrays)
    return pl.pallas_call(
        publish_kernel,
        out_shape=tuple(jax.ShapeDtypeStruct(a.shape, a.dtype) for a in stepped),
        in_specs=[vmem, vmem],
        out_specs=(hbm, hbm),
        scratch_shapes=[dma((2,))],
        compiler_params=pltpu.CompilerParams(vmem_limit_bytes=4 << 20),
    )(*stepped)


def solution(mesh):
    placed = (P(None, "gz", None, "gx"), P(None, "gz", None, "gx"), P())
    return jax.shard_map(
        per_device,
        mesh=mesh,
        in_specs=placed,
        out_specs=(P(None, "gz", None, "gx"), P("gz", None, "gx")),
        check_vma=False,
    )
```

```python
import math

import jax
import jax.numpy as jnp
import numpy as np
from jax import lax
from jax.experimental import pallas as pl
from jax.experimental.pallas import tpu as pltpu
from jax.sharding import PartitionSpec as P

TIME_STEP = 0.4
ADVECT_WEIGHT = 5.0 / 12.0
EARLIER_WEIGHT = -17.0 / 60.0
VISCOUS_WEIGHT = 2.0 / 15.0
NX = 512
NY = 256
NZ = 64
LANES = 128
PEERS = 256
LOGICAL = pl.DeviceIdType.LOGICAL
F32 = jnp.float32
BF16 = jnp.bfloat16
NN = (((1,), (0,)), ((), ()))
NT = (((1,), (1,)), ((), ()))
TN = (((0,), (0,)), ((), ()))


def hops(shift):
    return min(shift[0], 4 - shift[0]) + min(shift[1], 4 - shift[1]) + min(shift[2], 8 - shift[2])


SHIFTS = sorted(
    (
        (i, k, j, m)
        for m in (1, 0)
        for j in (4, 3, 5, 2, 6, 1, 7, 0)
        for k in (2, 1, 3, 0)
        for i in (2, 1, 3, 0)
        if (i, k, j, m) != (0, 0, 0, 0)
    ),
    key=lambda shift: -hops(shift),
)


def cosine_table(extent):
    wavenumber = np.arange(extent)[:, None]
    points = np.arange(extent)[None, :]
    residue = wavenumber * (2 * points + 1) % (4 * extent)
    cosines = np.cos(residue * (math.pi / (2 * extent))) * math.sqrt(2.0 / extent)
    cosines[0] *= math.sqrt(0.5)
    return cosines


def halves(table):
    high = table.astype(np.float32).astype(jnp.bfloat16)
    low = (table - high.astype(np.float64)).astype(np.float32).astype(jnp.bfloat16)
    return np.stack([high, low])


def split(values):
    high = values.astype(BF16)
    low = (values - high.astype(F32)).astype(BF16)
    return high, low


def mul(a, b, dims):
    return lax.dot_general(a, b, dims, preferred_element_type=F32)


def table_times(table, values):
    high, low = split(values)
    t_high, t_low = table[0], table[1]
    return mul(t_high, high, NN) + (mul(t_high, low, NN) + mul(t_low, high, NN))


def times_table(values, table, dims):
    high, low = split(values)
    t_high, t_low = table[0], table[1]
    return mul(high, t_high, dims) + (mul(high, t_low, dims) + mul(low, t_high, dims))


def row_ids(shape):
    return lax.broadcasted_iota(jnp.int32, shape, 0)


def lane_ids(shape):
    return lax.broadcasted_iota(jnp.int32, shape, 1)


def y_neighbours(field):
    rows = row_ids(field.shape)
    count = field.shape[0]
    after = jnp.where(rows == count - 1, field, pltpu.roll(field, count - 1, 0))
    before = jnp.where(rows == 0, field, pltpu.roll(field, 1, 0))
    return after, before


def z_slope(columns, metric):
    rows = row_ids(columns.shape)
    count = columns.shape[0]
    after = jnp.where(rows == count - 1, 0.0, pltpu.roll(columns, count - 1, 0))
    before = jnp.where(rows == 0, 0.0, pltpu.roll(columns, 1, 0))
    return metric * (0.5 * (after - before))


def x_slope(lines):
    count = lines.shape[1]
    return 0.5 * (pltpu.roll(lines, count - 1, 1) - pltpu.roll(lines, 1, 1))


def lined_x(field, edge_rows):
    shape = (16, LANES)
    places = (row_ids(shape) == 1) & (lane_ids(shape) == 0)
    places |= (row_ids(shape) == 8) & (lane_ids(shape) == LANES - 1)
    places = places.astype(F32).astype(BF16)
    high, low = split(edge_rows)
    outer = mul(high, places, TN) + mul(low, places, TN)
    lanes = lane_ids(field.shape)
    after = jnp.where(lanes == LANES - 1, outer, pltpu.roll(field, LANES - 1, 1))
    before = jnp.where(lanes == 0, outer, pltpu.roll(field, 1, 1))
    return after, before


def edge_lines(field):
    shape = (8, LANES)
    picks = (row_ids(shape) == 0) & (lane_ids(shape) == 0)
    picks |= (row_ids(shape) == 1) & (lane_ids(shape) == LANES - 1)
    picks = picks.astype(F32).astype(BF16)
    high, low = split(field)
    return mul(picks, high, NT) + mul(picks, low, NT)


def step_kernel(
    faces,
    velocity_in,
    earlier_in,
    y_second_in,
    y_forward_in,
    y_inverse_in,
    x_table_in,
    new_velocity,
    pressure,
    velocity,
    earlier,
    y_second,
    y_forward,
    y_inverse,
    x_table,
    edges,
    edges_in,
    edges_z,
    below,
    above,
    partial,
    y_rows,
    gathered,
    metrics,
    factor_c,
    factor_a,
    factor_b,
    middle,
    spread,
    returned,
    load_sem,
    edge_send,
    edge_recv,
    halo_send,
    halo_recv,
    out_send,
    out_recv,
    back_send,
    back_recv,
    plane_token,
    line_token,
):
    loads = [
        pltpu.make_async_copy(source, target, load_sem.at[i])
        for i, (source, target) in enumerate(
            (
                (velocity_in.at[0], velocity.at[0]),
                (velocity_in.at[2], velocity.at[2]),
                (velocity_in.at[1], velocity.at[1]),
                (y_second_in, y_second),
                (earlier_in, earlier),
                (y_forward_in, y_forward),
                (x_table_in, x_table),
                (y_inverse_in, y_inverse),
            )
        )
    ]
    for load in loads[:3]:
        load.start()

    group = lax.axis_index("gx")
    layer = lax.axis_index("gz")
    me = group * 64 + layer
    y_parts = [((layer & 6) + (shift << 1)) & 6 for shift in range(4)]
    core_parts = [layer & 1, (layer & 1) ^ 1]
    x_parts = [(group + shift) & 3 for shift in range(4)]
    x_line = [x_parts[i] * 64 + layer for i in (1, 3, 2)]
    y_line = [
        group * 64 + ((layer & 56) | (y_parts[k] | core_parts[m]))
        for k, m in ((0, 1), (1, 0), (1, 1), (3, 0), (3, 1), (2, 0), (2, 1))
    ]
    z_line = [
        group * 64 + (((layer & 56) + (shift << 3)) & 56) + (layer & 7)
        for shift in (1, 7, 2, 6, 3, 5, 4)
    ]
    x_right, x_left = x_line[0], x_line[1]
    z_up = group * 64 + ((layer + 1) & 63)
    z_down = group * 64 + ((layer + 63) & 63)
    at_top = (layer & 7) == 7
    at_bottom = (layer & 7) == 0

    def tell(sem, peer):
        pl.semaphore_signal(sem, inc=1, device_id=peer, device_id_type=LOGICAL)

    z_parts = [((layer & 56) + (shift << 3)) & 56 for shift in range(8)]

    def each_peer(act):
        for i, k, j, m in SHIFTS:
            act(x_parts[i], z_parts[j] | (y_parts[k] | core_parts[m]))

    def remote(source, target, send, recv, peer):
        return pltpu.make_async_remote_copy(
            src_ref=source,
            dst_ref=target,
            send_sem=send,
            recv_sem=recv,
            device_id=peer,
            device_id_type=LOGICAL,
        )

    barrier = pltpu.get_barrier_semaphore()

    @pl.when(at_top)
    def _():
        tell(barrier, z_up)

    @pl.when(at_bottom)
    def _():
        tell(barrier, z_down)

    for peer in y_line + x_line + z_line:
        tell(barrier, peer)
    for i in range(3):
        loads[i].wait()
    for load in loads[3:]:
        load.start()
    for c in range(3):
        edges[0, :, c * NY : c * NY + NY] = edge_lines(velocity[c, 0])
    pl.semaphore_wait(
        barrier, 17 + jnp.where(at_top, 1, 0) + jnp.where(at_bottom, 1, 0)
    )

    def send_edges(k, width):
        copies = []
        for side, peer in enumerate((x_right, x_left)):
            copies.append(
                remote(
                    edges.at[k, :, pl.ds(0, width)],
                    edges_in.at[k, side, :, pl.ds(0, width)],
                    edge_send.at[k, side],
                    edge_recv.at[k, side],
                    peer,
                )
            )
            copies[-1].start()
        return copies

    def edge_pair(k, first):
        part = slice(first, first + NY)
        return jnp.concatenate([edges_in[k, 0, :, part], edges_in[k, 1, :, part]], 0)

    velocity_edges = send_edges(0, 3 * NY)
    layer_edges = []
    for side, peer in enumerate((z_up, z_down)):
        layer_edges.append(
            remote(
                edges.at[0], edges_z.at[side], edge_send.at[3, side], edge_recv.at[3, side], peer
            )
        )
        layer_edges[-1].start()
    halos = {}
    for c in (2, 0, 1):
        up = remote(velocity.at[c, 0], below.at[c], halo_send.at[0, c], halo_recv.at[0, c], z_up)
        down = remote(velocity.at[c, 0], above.at[c], halo_send.at[1, c], halo_recv.at[1, c], z_down)
        up.start()
        down.start()
        halos[c] = (up, down)
    for peer in y_line:
        tell(plane_token, peer)

    u = velocity[0, 0]
    v = velocity[1, 0]
    loads[3].wait()
    loads[4].wait()
    for c in (0, 2, 1):
        field = velocity[c, 0]
        after, before = y_neighbours(field)
        bend = table_times(y_second, field) - 2.0 * field
        partial[c] = field + TIME_STEP * (
            EARLIER_WEIGHT * earlier[c, 0].astype(F32)
            + VISCOUS_WEIGHT * bend
            - ADVECT_WEIGHT * (v * (0.5 * (after - before)))
        )

    pl.semaphore_wait(plane_token, 7)
    for peer in x_line:
        tell(line_token, peer)

    lower = faces[0, layer]
    upper = faces[1, layer]
    metric = 0.5 * (lower + upper)
    w = velocity[2, 0]

    def with_z(base, field, below_it, above_it, drift):
        after = jnp.where(layer == NZ - 1, 0.0, above_it)
        before = jnp.where(layer == 0, 0.0, below_it)
        bend = metric * (upper * (after - field) - lower * (field - before))
        return base + TIME_STEP * (
            VISCOUS_WEIGHT * bend - ADVECT_WEIGHT * (drift * (metric * (0.5 * (after - before))))
        )

    def add_x(c):
        after, before = lined_x(velocity[c, 0], edge_pair(0, c * NY))
        partial[c] = partial[c] + TIME_STEP * (
            VISCOUS_WEIGHT * (after + before) - ADVECT_WEIGHT * (u * (0.5 * (after - before)))
        )

    def predict(c):
        for copy in halos[c]:
            copy.wait()
        predicted = with_z(partial[c], velocity[c, 0], below[c], above[c], w)
        partial[c] = predicted
        return predicted

    for copy in velocity_edges:
        copy.wait()
    add_x(0)
    own = edge_lines(partial[0])
    for copy in layer_edges:
        copy.wait()
    edges[1, :, :NY] = with_z(
        own,
        edges[0, :, :NY],
        edges_z[0, :, :NY],
        edges_z[1, :, :NY],
        edges[0, :, 2 * NY :],
    )
    u_edges = send_edges(1, NY)
    add_x(2)
    add_x(1)
    loads[5].wait()

    def send_rows(slot, field):
        y_rows[slot] = table_times(y_forward, field)

        def send(px, pz):
            peer = px * 64 + pz
            remote(
                y_rows.at[slot, pl.ds(peer, 1)],
                gathered.at[slot, group, pl.ds(layer, 1)],
                out_send.at[slot],
                out_recv.at[slot],
                peer,
            ).start()

        each_peer(send)
        gathered[slot, group, pl.ds(layer, 1)] = y_rows[slot, pl.ds(me, 1)]

    predicted_w = predict(2)
    pl.semaphore_wait(line_token, 3)
    send_rows(0, predicted_w)
    predicted_u = predict(0)
    for copy in u_edges:
        copy.wait()
    after, before = lined_x(predicted_u, edge_pair(1, 0))
    flow = after - before
    after, before = y_neighbours(predict(1))
    send_rows(1, 0.5 * (flow + (after - before)))

    k_y = me.astype(F32) * (math.pi / NY)
    k_x = lane_ids((1, NX)).astype(F32) * (math.pi / NX)
    eigen = k_y * k_y + k_x * k_x

    def factor_row(z, ratio, inner, outer):
        total = faces[0, z] + faces[1, z]
        metrics[pl.ds(z, 1)] = jnp.full((1, LANES), 0.5 * total, F32)
        per_metric = 2.0 / jnp.full((1, NX), total, F32)
        inverse = 1.0 / (-total - eigen * per_metric - inner * ratio)
        ratio = outer * inverse
        factor_c[pl.ds(z, 1)] = ratio
        factor_a[pl.ds(z, 1)] = inner * inverse
        factor_b[pl.ds(z, 1)] = (per_metric * inverse) * (1.0 / TIME_STEP)
        return ratio

    half = NZ // 2
    low_ratio = jnp.zeros((1, NX), F32)
    high_ratio = jnp.zeros((1, NX), F32)
    for z in range(half):
        low_ratio = factor_row(z, low_ratio, faces[0, z], faces[1, z])
        mirror = NZ - 1 - z
        high_ratio = factor_row(mirror, high_ratio, faces[1, mirror], faces[0, mirror])
    middle[...] = 1.0 / (1.0 - low_ratio * high_ratio)
    metric_rows = jnp.concatenate([metrics[...]] * 4, 1)
    loads[6].wait()
    loads[7].wait()

    others = returned.at[0, pl.ds(0, PEERS - 1)]

    def finish(sem):
        pltpu.make_async_copy(others, others, sem).wait()

    def lines(slot):
        return jnp.concatenate([gathered[slot, part] for part in range(4)], 1)

    finish(out_recv.at[0])
    source = z_slope(lines(0), metric_rows)
    finish(out_recv.at[1])
    source = source + lines(1)
    factor_b[...] = factor_b[...] * times_table(source, x_table, NT)
    low = jnp.zeros((1, NX), F32)
    high = jnp.zeros((1, NX), F32)
    for z in range(half):
        mirror = NZ - 1 - z
        low = factor_b[pl.ds(z, 1)] - factor_a[pl.ds(z, 1)] * low
        high = factor_b[pl.ds(mirror, 1)] - factor_a[pl.ds(mirror, 1)] * high
        factor_b[pl.ds(z, 1)] = low
        factor_b[pl.ds(mirror, 1)] = high
    low = (low - factor_c[pl.ds(half - 1, 1)] * high) * middle[...]
    high = high - factor_c[pl.ds(half, 1)] * low
    factor_b[pl.ds(half - 1, 1)] = low
    factor_b[pl.ds(half, 1)] = high
    for z in reversed(range(half - 1)):
        mirror = NZ - 1 - z
        low = factor_b[pl.ds(z, 1)] - factor_c[pl.ds(z, 1)] * low
        high = factor_b[pl.ds(mirror, 1)] - factor_c[pl.ds(mirror, 1)] * high
        factor_b[pl.ds(z, 1)] = low
        factor_b[pl.ds(mirror, 1)] = high
    solved = times_table(factor_b[...], x_table, NN)
    for slot in range(2):
        lined = z_slope(solved, metric_rows) if slot else solved
        for part in range(4):
            spread[slot, part] = lined[:, part * LANES : part * LANES + LANES]

        def send_back(px, pz):
            remote(
                spread.at[slot, px, pl.ds(pz, 1)],
                returned.at[slot, pl.ds(me, 1)],
                back_send.at[slot],
                back_recv.at[slot],
                px * 64 + pz,
            ).start()

        each_peer(send_back)
        returned[slot, pl.ds(me, 1)] = spread[slot, group, pl.ds(layer, 1)]

    finish(back_recv.at[0])
    rows = returned[0]
    edges[2, :, :NY] = edge_lines(rows)
    p_edges = send_edges(2, NY)
    field = table_times(y_inverse, rows)
    pressure[0] = field
    lanes = lane_ids(rows.shape)
    after = jnp.where(lanes == LANES - 1, 0.0, pltpu.roll(rows, LANES - 1, 1))
    before = jnp.where(lanes == 0, 0.0, pltpu.roll(rows, 1, 1))
    inner_slope = table_times(y_inverse, 0.5 * (after - before))
    after, before = y_neighbours(field)
    new_velocity[1, 0] = partial[1] - (0.5 * TIME_STEP) * (after - before)
    finish(back_recv.at[1])
    new_velocity[2, 0] = partial[2] - TIME_STEP * table_times(y_inverse, returned[1])
    for copy in p_edges:
        copy.wait()
    shape = (16, LANES)
    places = jnp.where((row_ids(shape) == 8) & (lane_ids(shape) == LANES - 1), 0.5, 0.0)
    places = jnp.where((row_ids(shape) == 1) & (lane_ids(shape) == 0), -0.5, places).astype(BF16)
    high, low = split(times_table(edge_pair(2, 0), y_inverse, NT))
    slope = inner_slope + (mul(high, places, TN) + mul(low, places, TN))
    new_velocity[0, 0] = partial[0] - TIME_STEP * slope
    for slot in range(2):
        finish(out_send.at[slot])
        finish(back_send.at[slot])


def publish_kernel(step_in, pressure_in, step_out, pressure_out, sems):
    copies = (
        pltpu.make_async_copy(step_in, step_out, sems.at[0]),
        pltpu.make_async_copy(pressure_in, pressure_out, sems.at[1]),
    )
    for copy in copies:
        copy.start()
    for copy in copies:
        copy.wait()


def per_device(velocity, earlier_term, face_metric):
    y_cosines = cosine_table(NY)
    y_squares = (np.arange(NY) * (math.pi / NY)) ** 2
    y_second = -(y_cosines.T * y_squares) @ y_cosines
    vmem = pl.BlockSpec(memory_space=pltpu.VMEM)
    hbm = pl.BlockSpec(memory_space=pltpu.HBM)
    dma = pltpu.SemaphoreType.DMA
    arrays = [
        pltpu.with_memory_space_constraint(array, pltpu.HBM)
        for array in (
            velocity,
            earlier_term,
            jnp.asarray(halves(y_second)),
            jnp.asarray(halves(y_cosines)),
            jnp.asarray(halves(y_cosines.T)),
            jnp.asarray(halves(cosine_table(NX))),
        )
    ]
    stepped = pl.pallas_call(
        step_kernel,
        out_shape=(
            jax.ShapeDtypeStruct(velocity.shape, F32),
            jax.ShapeDtypeStruct(velocity.shape[1:], F32),
        ),
        in_specs=[pl.BlockSpec(memory_space=pltpu.SMEM)] + [hbm] * 6,
        out_specs=(vmem, vmem),
        scratch_shapes=[
            pltpu.VMEM((3, 1, NY, LANES), F32),
            pltpu.VMEM((3, 1, NY, LANES), BF16),
            pltpu.VMEM((2, NY, NY), BF16),
            pltpu.VMEM((2, NY, NY), BF16),
            pltpu.VMEM((2, NY, NY), BF16),
            pltpu.VMEM((2, NX, NX), BF16),
            pltpu.VMEM((3, 8, 3 * NY), F32),
            pltpu.VMEM((3, 2, 8, 3 * NY), F32),
            pltpu.VMEM((2, 8, 3 * NY), F32),
            pltpu.VMEM((3, NY, LANES), F32),
            pltpu.VMEM((3, NY, LANES), F32),
            pltpu.VMEM((3, NY, LANES), F32),
            pltpu.VMEM((2, NY, LANES), F32),
            pltpu.VMEM((2, 4, NZ, LANES), F32),
            pltpu.VMEM((NZ, LANES), F32),
            pltpu.VMEM((NZ, NX), F32),
            pltpu.VMEM((NZ, NX), F32),
            pltpu.VMEM((NZ, NX), F32),
            pltpu.VMEM((1, NX), F32),
            pltpu.VMEM((2, 4, NZ, LANES), F32),
            pltpu.VMEM((2, NY, LANES), F32),
            dma((8,)),
            dma((4, 2)),
            dma((4, 2)),
            dma((2, 3)),
            dma((2, 3)),
            dma((2,)),
            dma((2,)),
            dma((2,)),
            dma((2,)),
            pltpu.SemaphoreType.REGULAR,
            pltpu.SemaphoreType.REGULAR,
        ],
        compiler_params=pltpu.CompilerParams(
            collective_id=0, has_side_effects=True, vmem_limit_bytes=16 << 20
        ),
    )(pltpu.with_memory_space_constraint(face_metric, pltpu.HBM), *arrays)
    return pl.pallas_call(
        publish_kernel,
        out_shape=tuple(jax.ShapeDtypeStruct(a.shape, a.dtype) for a in stepped),
        in_specs=[vmem, vmem],
        out_specs=(hbm, hbm),
        scratch_shapes=[dma((2,))],
        compiler_params=pltpu.CompilerParams(vmem_limit_bytes=4 << 20),
    )(*stepped)


def solution(mesh):
    placed = (P(None, "gz", None, "gx"), P(None, "gz", None, "gx"), P())
    return jax.shard_map(
        per_device,
        mesh=mesh,
        in_specs=placed,
        out_specs=(P(None, "gz", None, "gx"), P("gz", None, "gx")),
        check_vma=False,
    )
```
